16 devices in a mesh: dp: 2 (over y, z), tp: 8 (over x, core).
Axes of the slice: x: 4, y: 2, z: 1, core: 2. Of those that a mesh axis runs over, the one named last changes fastest.
The devices are a block of a 4x4x8 slice.
Arguments:
- patches: bfloat16 [64, 256, 588], P('dp', 'tp'), parts along dimension 0
- patch_w: bfloat16 [588, 1152], replicated
- patch_b: bfloat16 [1152], replicated
- pos_emb: bfloat16 [256, 1152], P('tp')
- ln_scale: bfloat16 [2, 1152], replicated
- ln_bias: bfloat16 [2, 1152], replicated
- qkv_w: bfloat16 [3, 1152, 16, 72], P(None, None, 'tp')
- qkv_b: bfloat16 [3, 16, 72], P(None, 'tp')
- out_w: bfloat16 [16, 72, 1152], P('tp')
- out_b: bfloat16 [1152], replicated
- fc1_w: bfloat16 [1152, 4304], P(None, 'tp')
- fc1_b: bfloat16 [4304], P('tp')
- fc2_w: bfloat16 [4304, 1152], P('tp')
- fc2_b: bfloat16 [1152], replicated
- d_out: bfloat16 [64, 256, 1152], P('dp', 'tp'), parts along dimension 0
Outputs:
- output 1: bfloat16 [64, 256, 1152], P('dp', 'tp'), parts along dimension 0
- output 2: bfloat16 [1176, 1152], P('dp'), parts along dimension 0
- output 3: bfloat16 [2304], P('dp'), parts along dimension 0
- output 4: bfloat16 [512, 1152], P(('dp', 'tp')), parts along dimension 0
- output 5: bfloat16 [4, 1152], P('dp'), parts along dimension 0
- output 6: bfloat16 [4, 1152], P('dp'), parts along dimension 0
- output 7: bfloat16 [6, 1152, 16, 72], P('dp', None, 'tp'), parts along dimension 0
- output 8: bfloat16 [6, 16, 72], P('dp', 'tp'), parts along dimension 0
- output 9: bfloat16 [32, 72, 1152], P(('dp', 'tp')), parts along dimension 0
- output 10: bfloat16 [2304], P('dp'), parts along dimension 0
- output 11: bfloat16 [2304, 4304], P('dp', 'tp'), parts along dimension 0
- output 12: bfloat16 [8608], P(('dp', 'tp')), parts along dimension 0
- output 13: bfloat16 [8608, 1152], P(('dp', 'tp')), parts along dimension 0
- output 14: bfloat16 [2304], P('dp'), parts along dimension 0
There are 2 independent parts. The reference program is written for one: setup_inputs(seed, part) draws one part's arguments, and reference() takes and returns one part's arrays. A program takes and returns all parts, laid end to end along the dimension named above; an argument that names none is the same for every part.
All inputs are finite; a program needn't handle non-finite values.
Results may differ from the reference program's by a relative error of at most 0.0181147.
Values are sent between devices in bfloat16 or wider.
A program may use at most 768 MiB of HBM per device.

```python
import functools
import jax
import jax.numpy as jnp
from jax import lax

NUM_IMAGES = 32
NUM_TOKENS = 256
PATCH_DIM = 588
MODEL_DIM = 1152
NUM_HEADS = 16
HEAD_DIM = 72
MLP_DIM = 4304
LN_EPS = 1e-6


def draw_normal(key, shape, scale):
    return (jax.random.normal(key, shape, jnp.float32) * scale).astype(jnp.bfloat16)


def setup_inputs(seed: int = 0, part: int = 0) -> dict:
    base_key = jax.random.key(seed)
    part_key = jax.random.fold_in(base_key, part)
    weight_keys = jax.random.split(base_key, 13)
    data_keys = jax.random.split(part_key, 2)
    qk_gain = 1.6 * MODEL_DIM ** -0.5
    qkv_gain = jnp.array([qk_gain, qk_gain, MODEL_DIM ** -0.5], jnp.float32).reshape(3, 1, 1, 1)
    ln_gain = 1.0 + 0.3 * jax.random.normal(weight_keys[3], (2, MODEL_DIM), jnp.float32)
    qkv_raw = jax.random.normal(weight_keys[5], (3, MODEL_DIM, NUM_HEADS, HEAD_DIM), jnp.float32)
    return {
        'patches': draw_normal(data_keys[0], (NUM_IMAGES, NUM_TOKENS, PATCH_DIM), 1.0),
        'patch_w': draw_normal(weight_keys[0], (PATCH_DIM, MODEL_DIM), PATCH_DIM ** -0.5),
        'patch_b': draw_normal(weight_keys[1], (MODEL_DIM,), 0.5),
        'pos_emb': draw_normal(weight_keys[2], (NUM_TOKENS, MODEL_DIM), 0.5),
        'ln_scale': ln_gain.astype(jnp.bfloat16),
        'ln_bias': draw_normal(weight_keys[4], (2, MODEL_DIM), 0.3),
        'qkv_w': (qkv_raw * qkv_gain).astype(jnp.bfloat16),
        'qkv_b': draw_normal(weight_keys[6], (3, NUM_HEADS, HEAD_DIM), 0.3),
        'out_w': draw_normal(weight_keys[7], (NUM_HEADS, HEAD_DIM, MODEL_DIM), MODEL_DIM ** -0.5),
        'out_b': draw_normal(weight_keys[8], (MODEL_DIM,), 0.5),
        'fc1_w': draw_normal(weight_keys[9], (MODEL_DIM, MLP_DIM), MODEL_DIM ** -0.5),
        'fc1_b': draw_normal(weight_keys[10], (MLP_DIM,), 0.5),
        'fc2_w': draw_normal(weight_keys[11], (MLP_DIM, MODEL_DIM), MLP_DIM ** -0.5),
        'fc2_b': draw_normal(weight_keys[12], (MODEL_DIM,), 0.5),
        'd_out': draw_normal(data_keys[1], (NUM_IMAGES, NUM_TOKENS, MODEL_DIM), 1.0),
    }


def layer_norm(x_val, scale, bias):
    row_mean = jnp.mean(x_val, axis=-1, keepdims=True)
    centered = x_val - row_mean
    row_var = jnp.mean(centered * centered, axis=-1, keepdims=True)
    return centered * lax.rsqrt(row_var + LN_EPS) * scale.astype(jnp.float32) + bias.astype(jnp.float32)


def attend_image(qkv_img):
    query = qkv_img[:, 0].astype(jnp.float32)
    keys_img = qkv_img[:, 1].astype(jnp.float32)
    values = qkv_img[:, 2].astype(jnp.float32)
    scores = jnp.einsum('qhc,khc->hqk', query, keys_img) * HEAD_DIM ** -0.5
    probs = jax.nn.softmax(scores, axis=-1).astype(jnp.bfloat16)
    context = jnp.einsum('hqk,khc->qhc', probs.astype(jnp.float32), values)
    return context.astype(jnp.bfloat16)


def forward(patches, params):
    patch_w, patch_b, pos_emb, ln_scale, ln_bias, qkv_w, qkv_b, out_w, out_b, fc1_w, fc1_b, fc2_w, fc2_b = params
    emb = jnp.einsum('btp,pd->btd', patches.astype(jnp.float32), patch_w.astype(jnp.float32))
    emb_f = (emb + patch_b.astype(jnp.float32) + pos_emb.astype(jnp.float32)).astype(jnp.bfloat16).astype(jnp.float32)
    h_one = layer_norm(emb_f, ln_scale[0], ln_bias[0]).astype(jnp.bfloat16)
    qkv = jnp.einsum('btd,sdhc->btshc', h_one.astype(jnp.float32), qkv_w.astype(jnp.float32)) + qkv_b.astype(jnp.float32)
    context = lax.map(jax.checkpoint(attend_image), qkv.astype(jnp.bfloat16))
    attn_out = jnp.einsum('bthc,hcd->btd', context.astype(jnp.float32), out_w.astype(jnp.float32)) + out_b.astype(jnp.float32)
    x_one_f = (emb_f + attn_out).astype(jnp.bfloat16).astype(jnp.float32)
    h_two = layer_norm(x_one_f, ln_scale[1], ln_bias[1]).astype(jnp.bfloat16)
    pre_act = jnp.einsum('btd,df->btf', h_two.astype(jnp.float32), fc1_w.astype(jnp.float32)) + fc1_b.astype(jnp.float32)
    hidden = jax.nn.gelu(pre_act, approximate=True).astype(jnp.bfloat16)
    mlp_out = jnp.einsum('btf,fd->btd', hidden.astype(jnp.float32), fc2_w.astype(jnp.float32)) + fc2_b.astype(jnp.float32)
    return (x_one_f + mlp_out).astype(jnp.bfloat16)


def reference(patches, patch_w, patch_b, pos_emb, ln_scale, ln_bias, qkv_w, qkv_b, out_w, out_b, fc1_w, fc1_b, fc2_w, fc2_b, d_out):
    params = (patch_w, patch_b, pos_emb, ln_scale, ln_bias, qkv_w, qkv_b, out_w, out_b, fc1_w, fc1_b, fc2_w, fc2_b)
    x_two, pull_back = jax.vjp(functools.partial(forward, patches), params)
    grads = pull_back(d_out)[0]
    return (x_two, grads[0], grads[1], grads[2], grads[3], grads[4], grads[5], grads[6], grads[7], grads[8], grads[9], grads[10], grads[11], grads[12])
```

```python
import functools

import jax
import jax.numpy as jnp
from jax import lax
from jax.experimental import pallas as pl
from jax.experimental.pallas import tpu as pltpu
from jax.sharding import PartitionSpec as P

LN_EPS = 1e-6
WIDE = jnp.float32
HALF = jnp.bfloat16


def layer_norm(x_val, scale_f, bias_f):
    row_mean = jnp.mean(x_val, axis=-1, keepdims=True)
    centered = x_val - row_mean
    row_var = jnp.mean(centered * centered, axis=-1, keepdims=True)
    return centered * lax.rsqrt(row_var + LN_EPS) * scale_f + bias_f


def gelu_tanh(pre_act):
    return jax.nn.gelu(pre_act, approximate=True)


def dot(a_val, b_val, contract):
    return lax.dot_general(a_val, b_val, ((contract[0], contract[1]), ((), ())), preferred_element_type=WIDE)


def attention_forward_kernel(heads, scale, qkv_ref, out_ref):
    width = qkv_ref.shape[-1] // heads
    for head in range(heads):
        cols = slice(head * width, (head + 1) * width)
        query, keys, values = (qkv_ref[part, :, 0, :, cols].reshape(-1, width) for part in range(3))
        scores = dot(query, keys, ((1,), (1,))) * scale
        scores = jnp.exp(scores - jnp.max(scores, axis=1, keepdims=True))
        probs = scores * (1.0 / jnp.sum(scores, axis=1, keepdims=True))
        context = dot(probs.astype(HALF), values, ((1,), (0,))).astype(HALF)
        out_ref[:, 0, :, cols] = context.reshape(out_ref.shape[0], -1, width)


def attention_backward_kernel(heads, scale, qkv_ref, d_ref, out_ref):
    width = qkv_ref.shape[-1] // heads
    for head in range(heads):
        cols = slice(head * width, (head + 1) * width)
        query, keys, values = (qkv_ref[part, :, 0, :, cols].reshape(-1, width) for part in range(3))
        d_context = d_ref[:, 0, :, cols].reshape(-1, width)
        scores = dot(keys, query, ((1,), (1,))) * scale
        scores = jnp.exp(scores - jnp.max(scores, axis=0, keepdims=True))
        probs = scores * (1.0 / jnp.sum(scores, axis=0, keepdims=True))
        d_probs = dot(values, d_context, ((1,), (1,))).astype(HALF).astype(WIDE)
        d_scores = probs * (d_probs - jnp.sum(d_probs * probs, axis=0, keepdims=True))
        d_scores = (d_scores * scale).astype(HALF)
        d_values = dot(probs.astype(HALF), d_context, ((1,), (0,))).astype(HALF)
        d_keys = dot(d_scores, query, ((1,), (0,))).astype(HALF)
        d_query = dot(d_scores, keys, ((0,), (0,))).astype(HALF)
        for part, grad in enumerate((d_query, d_keys, d_values)):
            out_ref[part, :, 0, :, cols] = grad.reshape(out_ref.shape[1], -1, width)


def attention_cost(images, heads, tokens, width, dots):
    return pl.CostEstimate(
        flops=2 * dots * images * heads * tokens * tokens * width,
        bytes_accessed=2 * (dots + 2) * images * heads * tokens * width,
        transcendentals=images * heads * tokens * tokens)


def attention_forward(qkv, heads, scale):
    _, blocks, images, rows, dim = qkv.shape
    return pl.pallas_call(
        functools.partial(attention_forward_kernel, heads, scale),
        out_shape=jax.ShapeDtypeStruct((blocks, images, rows, dim), HALF),
        grid=(images,),
        in_specs=[pl.BlockSpec((3, blocks, 1, rows, dim), lambda i: (0, 0, i, 0, 0))],
        out_specs=pl.BlockSpec((blocks, 1, rows, dim), lambda i: (0, i, 0, 0)),
        cost_estimate=attention_cost(images, heads, blocks * rows, dim // heads, 2),
        name='attention_forward',
    )(qkv)


def attention_backward(qkv, d_context, heads, scale):
    _, blocks, images, rows, dim = qkv.shape
    return pl.pallas_call(
        functools.partial(attention_backward_kernel, heads, scale),
        out_shape=jax.ShapeDtypeStruct(qkv.shape, HALF),
        grid=(images,),
        in_specs=[pl.BlockSpec((3, blocks, 1, rows, dim), lambda i: (0, 0, i, 0, 0)),
                  pl.BlockSpec((blocks, 1, rows, dim), lambda i: (0, i, 0, 0))],
        out_specs=pl.BlockSpec((3, blocks, 1, rows, dim), lambda i: (0, 0, i, 0, 0)),
        cost_estimate=attention_cost(images, heads, blocks * rows, dim // heads, 5),
        name='attention_backward',
    )(qkv, d_context)


def round_up(value, step):
    return (value + step - 1) // step * step


def pad_rows(x_val, rows):
    return jnp.pad(x_val, ((0, rows - x_val.shape[0]), (0, 0)))


def group_step(patches, patch_w, patch_b, pos_emb, ln_scale, ln_bias, qkv_w, qkv_b, out_w, out_b, fc1_w, fc1_b, fc2_w, fc2_b, d_out):
    size = lax.axis_size('tp')
    dim = patch_w.shape[1]
    heads_here, width = qkv_w.shape[2:]
    heads = heads_here * size
    head_rows = heads_here * width
    scale = width ** -0.5
    cols_here = fc1_w.shape[1]
    cols_pad = round_up(cols_here, 32)
    ln_scale_f = ln_scale.astype(WIDE)
    ln_bias_f = ln_bias.astype(WIDE)

    def images_of(x_val):
        x_val = x_val.reshape(size, -1, *x_val.shape[1:])
        return lax.all_to_all(x_val, 'tp', 0, 0, tiled=True)

    pos_rows = pos_emb.shape[0]
    biases = jnp.concatenate([qkv_b.reshape(-1), fc1_b])
    biases = jnp.pad(biases, (0, dim - biases.shape[0]))[None]
    tables = pad_rows(jnp.concatenate([pos_emb, biases]), round_up(pos_rows + 1, 16))
    patches_img = images_of(patches)
    tables = lax.all_gather(tables, 'tp', axis=0)
    pos_all = tables[:, :pos_rows]
    qkv_b_all = tables[:, pos_rows, :3 * head_rows].reshape(size, 3, head_rows).transpose(1, 0, 2).reshape(3, -1)
    fc1_b_all = tables[:, pos_rows, 3 * head_rows:3 * head_rows + cols_here]
    fc1_b_all = jnp.pad(fc1_b_all, ((0, 0), (0, cols_pad - cols_here))).reshape(-1)
    qkv_rows = qkv_w.transpose(0, 2, 3, 1).reshape(3, head_rows, dim)
    qkv_all = lax.all_gather(qkv_rows, 'tp', axis=1, tiled=True)
    out_all = lax.all_gather(out_w.reshape(head_rows, dim), 'tp', axis=0, tiled=True)
    fc1_all = lax.all_gather(pad_rows(fc1_w.T, cols_pad), 'tp', axis=0, tiled=True)
    d_out_img = images_of(d_out)
    fc2_all = lax.all_gather(pad_rows(fc2_w, cols_pad), 'tp', axis=0, tiled=True)

    emb = jnp.einsum('gbtp,pd->gbtd', patches_img, patch_w, preferred_element_type=WIDE)
    emb_f = (emb + patch_b.astype(WIDE) + pos_all[:, None].astype(WIDE)).astype(HALF).astype(WIDE)
    h_one_f, ln_one_vjp = jax.vjp(layer_norm, emb_f, ln_scale_f[0], ln_bias_f[0])
    h_one = h_one_f.astype(HALF)
    qkv = jnp.einsum('gbtd,snd->sgbtn', h_one, qkv_all, preferred_element_type=WIDE)
    qkv = (qkv + qkv_b_all.astype(WIDE)[:, None, None, None, :]).astype(HALF)
    context = attention_forward(qkv, heads, scale)
    attn_out = jnp.einsum('gbtn,nd->gbtd', context, out_all, preferred_element_type=WIDE)
    x_one_f = (emb_f + (attn_out + out_b.astype(WIDE))).astype(HALF).astype(WIDE)
    h_two_f, ln_two_vjp = jax.vjp(layer_norm, x_one_f, ln_scale_f[1], ln_bias_f[1])
    h_two = h_two_f.astype(HALF)
    pre_act = jnp.einsum('gbtd,fd->gbtf', h_two, fc1_all, preferred_element_type=WIDE) + fc1_b_all.astype(WIDE)
    hidden_f, gelu_vjp = jax.vjp(gelu_tanh, pre_act)
    hidden = hidden_f.astype(HALF)

    d_fc2_b = jnp.sum(d_out.astype(WIDE), axis=(0, 1))
    d_fc2_part = jnp.einsum('gbtf,gbtd->fd', hidden, d_out_img, preferred_element_type=WIDE)
    d_fc2_part, d_out_img, fc2_all, hidden = lax.optimization_barrier((d_fc2_part, d_out_img, fc2_all, hidden))
    d_fc2_w = lax.psum_scatter(d_fc2_part, 'tp', scatter_dimension=0, tiled=True)
    d_hidden = jnp.einsum('gbtd,fd->gbtf', d_out_img, fc2_all, preferred_element_type=WIDE).astype(HALF)
    d_pre = gelu_vjp(d_hidden.astype(WIDE))[0]
    d_fc1_b = jnp.sum(d_pre, axis=(0, 1, 2))
    d_pre_h = d_pre.astype(HALF)
    d_fc1_part = jnp.einsum('gbtf,gbtd->fd', d_pre_h, h_two, preferred_element_type=WIDE)
    d_fc1_part, d_pre_h, hidden = lax.optimization_barrier((d_fc1_part, d_pre_h, hidden))
    d_fc1_w = lax.psum_scatter(d_fc1_part, 'tp', scatter_dimension=0, tiled=True)
    mlp_out = jnp.einsum('gbtf,fd->gbtd', hidden, fc2_all, preferred_element_type=WIDE)
    x_two = (x_one_f + (mlp_out + fc2_b.astype(WIDE))).astype(HALF)
    x_two, d_pre_h = lax.optimization_barrier((x_two, d_pre_h))
    x_two = lax.all_to_all(x_two, 'tp', 0, 0, tiled=True).reshape(d_out.shape)
    d_h_two = jnp.einsum('gbtf,fd->gbtd', d_pre_h, fc1_all, preferred_element_type=WIDE).astype(HALF)
    d_x_ln, d_ln2_scale, d_ln2_bias = ln_two_vjp(d_h_two.astype(WIDE))
    d_x_one = (d_out_img.astype(WIDE) + d_x_ln).astype(HALF)
    d_out_b = jnp.sum(d_x_one, axis=(0, 1, 2), dtype=WIDE)
    d_out_part = jnp.einsum('gbtn,gbtd->nd', context, d_x_one, preferred_element_type=WIDE)
    d_out_part, d_x_one, d_fc2_w = lax.optimization_barrier((d_out_part, d_x_one, d_fc2_w))
    d_out_w = lax.psum_scatter(d_out_part, 'tp', scatter_dimension=0, tiled=True)
    d_context = jnp.einsum('gbtd,nd->gbtn', d_x_one, out_all, preferred_element_type=WIDE).astype(HALF)
    d_qkv = attention_backward(qkv, d_context, heads, scale)
    d_qkv_part = jnp.einsum('sgbtn,gbtd->snd', d_qkv, h_one, preferred_element_type=WIDE)
    d_qkv_part, d_qkv = lax.optimization_barrier((d_qkv_part, d_qkv))
    d_qkv_b = jnp.sum(d_qkv, axis=(1, 2, 3), dtype=WIDE)
    d_qkv_w = lax.psum_scatter(d_qkv_part, 'tp', scatter_dimension=1, tiled=True)
    d_h_one = jnp.einsum('sgbtn,snd->gbtd', d_qkv, qkv_all, preferred_element_type=WIDE).astype(HALF)
    d_h_one, d_fc1_w, x_two = lax.optimization_barrier((d_h_one, d_fc1_w, x_two))
    d_emb_ln, d_ln1_scale, d_ln1_bias = ln_one_vjp(d_h_one.astype(WIDE))
    d_emb = (d_x_one.astype(WIDE) + d_emb_ln).astype(HALF)
    d_pos = jnp.sum(d_emb, axis=1, dtype=WIDE)
    d_patch_b = jnp.sum(d_emb, axis=(0, 1, 2), dtype=WIDE)
    d_patch_w = jnp.einsum('gbtp,gbtd->pd', patches_img, d_emb, preferred_element_type=WIDE)

    shared = jnp.concatenate([d_patch_w, jnp.stack([d_patch_b, d_ln1_scale, d_ln2_scale, d_ln1_bias, d_ln2_bias, d_out_b, d_fc2_b])])
    shared_rows = shared.shape[0]
    shared = pad_rows(shared, round_up(shared_rows, 16 * size)).reshape(size, -1, dim)
    biases = jnp.concatenate([d_fc1_b.reshape(size, -1), d_qkv_b.reshape(3, size, -1).transpose(1, 0, 2).reshape(size, -1)], axis=1)
    biases = jnp.pad(biases, ((0, 0), (0, dim - biases.shape[1])))[:, None, :]
    biases = jnp.pad(biases, ((0, 0), (0, 7), (0, 0)))
    small = jnp.concatenate([d_pos, shared, biases], axis=1)
    small, d_out_w = lax.optimization_barrier((small, d_out_w))
    small = lax.psum_scatter(small, 'tp', scatter_dimension=0, tiled=True)[0]
    d_pos = small[:pos_rows].astype(HALF)
    d_fc1_b = small[-8, :cols_here]
    d_qkv_b = small[-8, cols_pad:cols_pad + 3 * head_rows].reshape(3, heads_here, width)
    shared = lax.all_gather(small[pos_rows:-8].astype(HALF), 'tp', axis=0, tiled=True)
    patch_rows = patch_w.shape[0]
    rest = shared[patch_rows:shared_rows]

    d_qkv_w = d_qkv_w.astype(HALF).reshape(3, heads_here, width, dim).transpose(0, 3, 1, 2)
    d_out_w = d_out_w.astype(HALF).reshape(heads_here, width, dim)
    d_fc1_w = d_fc1_w[:cols_here].astype(HALF).T
    d_fc2_w = d_fc2_w[:cols_here].astype(HALF)
    return (x_two, shared[:patch_rows], rest[0], d_pos, rest[1:3], rest[3:5], d_qkv_w, d_qkv_b.astype(HALF), d_out_w, rest[5], d_fc1_w, d_fc1_b.astype(HALF), d_fc2_w, rest[6])


def solution(mesh):
    in_specs = (P('dp', 'tp', None), P(), P(), P('tp', None), P(), P(), P(None, None, 'tp', None), P(None, 'tp', None), P('tp', None, None), P(), P(None, 'tp'), P('tp'), P('tp', None), P(), P('dp', 'tp', None))
    out_specs = (P('dp', 'tp', None), P('dp', None), P('dp'), P(('dp', 'tp'), None), P('dp', None), P('dp', None), P('dp', None, 'tp', None), P('dp', 'tp', None), P(('dp', 'tp'), None, None), P('dp'), P('dp', 'tp'), P(('dp', 'tp')), P(('dp', 'tp'), None), P('dp'))
    return jax.shard_map(group_step, mesh=mesh, in_specs=in_specs, out_specs=out_specs, check_vma=False)
```

```python
import functools

import jax
import jax.numpy as jnp
from jax import lax
from jax.experimental import pallas as pl
from jax.experimental.pallas import tpu as pltpu
from jax.sharding import PartitionSpec as P

LN_EPS = 1e-6
WIDE = jnp.float32
HALF = jnp.bfloat16


def layer_norm(x_val, scale_f, bias_f):
    row_mean = jnp.mean(x_val, axis=-1, keepdims=True)
    centered = x_val - row_mean
    row_var = jnp.mean(centered * centered, axis=-1, keepdims=True)
    return centered * lax.rsqrt(row_var + LN_EPS) * scale_f + bias_f


def gelu_tanh(pre_act):
    return jax.nn.gelu(pre_act, approximate=True)


def dot(a_val, b_val, contract):
    return lax.dot_general(a_val, b_val, ((contract[0], contract[1]), ((), ())), preferred_element_type=WIDE)


def attention_forward_kernel(heads, scale, qkv_ref, out_ref):
    width = qkv_ref.shape[-1] // heads
    for head in range(heads):
        cols = slice(head * width, (head + 1) * width)
        query, keys, values = (qkv_ref[part, :, 0, :, cols].reshape(-1, width) for part in range(3))
        scores = dot(keys, query, ((1,), (1,))) * scale
        scores = jnp.exp(scores - jnp.max(scores, axis=0, keepdims=True))
        probs = scores * (1.0 / jnp.sum(scores, axis=0, keepdims=True))
        context = dot(values, probs.astype(HALF), ((0,), (0,))).T.astype(HALF)
        out_ref[:, 0, :, cols] = context.reshape(out_ref.shape[0], -1, width)


def attention_backward_kernel(heads, scale, qkv_ref, d_ref, out_ref):
    width = qkv_ref.shape[-1] // heads
    for head in range(heads):
        cols = slice(head * width, (head + 1) * width)
        query, keys, values = (qkv_ref[part, :, 0, :, cols].reshape(-1, width) for part in range(3))
        d_context = d_ref[:, 0, :, cols].reshape(-1, width)
        scores = dot(keys, query, ((1,), (1,))) * scale
        scores = jnp.exp(scores - jnp.max(scores, axis=0, keepdims=True))
        probs = scores * (1.0 / jnp.sum(scores, axis=0, keepdims=True))
        d_probs = dot(values, d_context, ((1,), (1,))).astype(HALF).astype(WIDE)
        d_scores = probs * (d_probs - jnp.sum(d_probs * probs, axis=0, keepdims=True))
        d_scores = (d_scores * scale).astype(HALF)
        d_values = dot(probs.astype(HALF), d_context, ((1,), (0,))).astype(HALF)
        d_keys = dot(d_scores, query, ((1,), (0,))).astype(HALF)
        d_query = dot(keys, d_scores, ((0,), (0,))).T.astype(HALF)
        for part, grad in enumerate((d_query, d_keys, d_values)):
            out_ref[part, :, 0, :, cols] = grad.reshape(out_ref.shape[1], -1, width)


def attention_cost(images, heads, tokens, width, dots):
    return pl.CostEstimate(
        flops=2 * dots * images * heads * tokens * tokens * width,
        bytes_accessed=2 * (dots + 2) * images * heads * tokens * width,
        transcendentals=images * heads * tokens * tokens)


def attention_forward(qkv, heads, scale):
    _, blocks, images, rows, dim = qkv.shape
    return pl.pallas_call(
        functools.partial(attention_forward_kernel, heads, scale),
        out_shape=jax.ShapeDtypeStruct((blocks, images, rows, dim), HALF),
        grid=(images,),
        in_specs=[pl.BlockSpec((3, blocks, 1, rows, dim), lambda i: (0, 0, i, 0, 0))],
        out_specs=pl.BlockSpec((blocks, 1, rows, dim), lambda i: (0, i, 0, 0)),
        cost_estimate=attention_cost(images, heads, blocks * rows, dim // heads, 2),
        name='attention_forward',
    )(qkv)


def attention_backward(qkv, d_context, heads, scale):
    _, blocks, images, rows, dim = qkv.shape
    return pl.pallas_call(
        functools.partial(attention_backward_kernel, heads, scale),
        out_shape=jax.ShapeDtypeStruct(qkv.shape, HALF),
        grid=(images,),
        in_specs=[pl.BlockSpec((3, blocks, 1, rows, dim), lambda i: (0, 0, i, 0, 0)),
                  pl.BlockSpec((blocks, 1, rows, dim), lambda i: (0, i, 0, 0))],
        out_specs=pl.BlockSpec((3, blocks, 1, rows, dim), lambda i: (0, 0, i, 0, 0)),
        cost_estimate=attention_cost(images, heads, blocks * rows, dim // heads, 5),
        name='attention_backward',
    )(qkv, d_context)


def round_up(value, step):
    return (value + step - 1) // step * step


def pad_rows(x_val, rows):
    return jnp.pad(x_val, ((0, rows - x_val.shape[0]), (0, 0)))


def group_step(patches, patch_w, patch_b, pos_emb, ln_scale, ln_bias, qkv_w, qkv_b, out_w, out_b, fc1_w, fc1_b, fc2_w, fc2_b, d_out):
    size = lax.axis_size('tp')
    core = lax.rem(lax.axis_index('tp'), 2)
    same_core = [list(range(start, size, 2)) for start in range(2)]
    partner = [(index, index ^ 1) for index in range(size)]
    dim = patch_w.shape[1]
    heads_here, width = qkv_w.shape[2:]
    heads_half = heads_here * size // 2
    head_rows = heads_here * width
    scale = width ** -0.5
    cols_here = fc1_w.shape[1]
    cols_pad = round_up(cols_here, 32)
    ln_scale_f = ln_scale.astype(WIDE)
    ln_bias_f = ln_bias.astype(WIDE)
    tie = lax.optimization_barrier

    def images_of(x_val):
        x_val = x_val.reshape(size, -1, *x_val.shape[1:])
        return lax.all_to_all(x_val, 'tp', 0, 0, tiled=True)

    def gather(x_val, axis):
        return lax.all_gather(x_val, 'tp', axis=axis, tiled=True, axis_index_groups=same_core)

    def swap(x_val):
        return lax.ppermute(x_val, 'tp', partner)

    def scatter(x_val, axis):
        return lax.psum_scatter(x_val, 'tp', scatter_dimension=axis, tiled=True, axis_index_groups=same_core)

    def halves_of(table):
        table = table.reshape(size // 2, 2, *table.shape[1:])
        return [lax.dynamic_index_in_dim(table, index, 1, keepdims=False) for index in (core, 1 - core)]

    def product(spec, a_val, b_val):
        return jnp.einsum(spec, a_val, b_val, preferred_element_type=WIDE)

    def summed(spec, a_pair, b_pair):
        return product(spec, a_pair[0], b_pair[0]) + product(spec, a_pair[1], b_pair[1])

    pos_rows = pos_emb.shape[0]
    biases = jnp.concatenate([qkv_b.reshape(-1), fc1_b])
    biases = jnp.pad(biases, (0, dim - biases.shape[0]))[None]
    tables = pad_rows(jnp.concatenate([pos_emb, biases]), round_up(pos_rows + 1, 16))
    patches_img = images_of(patches)
    tables = lax.all_gather(tables, 'tp', axis=0)
    pos_all = tables[:, :pos_rows]
    qkv_b_all = [part.reshape(-1, 3, head_rows).transpose(1, 0, 2).reshape(3, 1, 1, 1, -1).astype(WIDE)
                 for part in halves_of(tables[:, pos_rows, :3 * head_rows])]
    fc1_b_all = [jnp.pad(part, ((0, 0), (0, cols_pad - cols_here))).reshape(-1).astype(WIDE)
                 for part in halves_of(tables[:, pos_rows, 3 * head_rows:3 * head_rows + cols_here])]
    qkv_own = gather(qkv_w.transpose(0, 2, 3, 1).reshape(3, head_rows, dim), 1)
    out_own = gather(out_w.reshape(head_rows, dim), 0)
    fc1_own = gather(pad_rows(fc1_w.T, cols_pad), 0)
    d_out_img = images_of(d_out)
    fc2_own = gather(pad_rows(fc2_w, cols_pad), 0)

    emb = product('gbtp,pd->gbtd', patches_img, patch_w)
    emb_f = (emb + patch_b.astype(WIDE) + pos_all[:, None].astype(WIDE)).astype(HALF).astype(WIDE)
    h_one_f, ln_one_vjp = jax.vjp(layer_norm, emb_f, ln_scale_f[0], ln_bias_f[0])
    h_one = h_one_f.astype(HALF)
    qkv_own, h_one = tie((qkv_own, h_one))
    qkv_all = [qkv_own, swap(qkv_own)]
    qkv = [(product('gbtd,snd->sgbtn', h_one, weight) + bias).astype(HALF) for weight, bias in zip(qkv_all, qkv_b_all)]
    out_own, qkv[0] = tie((out_own, qkv[0]))
    out_all = [out_own, swap(out_own)]
    context = [attention_forward(part, heads_half, scale) for part in qkv]
    attn_out = summed('gbtn,nd->gbtd', context, out_all)
    x_one_f = (emb_f + (attn_out + out_b.astype(WIDE))).astype(HALF).astype(WIDE)
    h_two_f, ln_two_vjp = jax.vjp(layer_norm, x_one_f, ln_scale_f[1], ln_bias_f[1])
    h_two = h_two_f.astype(HALF)
    fc1_own, h_two, d_out_img = tie((fc1_own, h_two, d_out_img))
    fc1_all = [fc1_own, swap(fc1_own)]
    hidden, gelu_vjps = [], []
    for weight, bias in zip(fc1_all, fc1_b_all):
        hidden_f, gelu_vjp = jax.vjp(gelu_tanh, product('gbtd,fd->gbtf', h_two, weight) + bias)
        hidden.append(hidden_f.astype(HALF))
        gelu_vjps.append(gelu_vjp)


    d_fc2_b = jnp.sum(d_out.astype(WIDE), axis=(0, 1))
    grad_fc2 = product('gbtf,gbtd->fd', hidden[1], d_out_img)
    fc2_own, grad_fc2, hidden[0] = tie((fc2_own, grad_fc2, hidden[0]))
    fc2_all = [fc2_own, swap(fc2_own)]
    grad_fc2 = product('gbtf,gbtd->fd', hidden[0], d_out_img) + swap(grad_fc2)
    grad_fc2, d_out_img, fc2_all, hidden = tie((grad_fc2, d_out_img, fc2_all, hidden))
    d_fc2_w = scatter(grad_fc2, 0)
    d_pre = [vjp(product('gbtd,fd->gbtf', d_out_img, weight).astype(HALF).astype(WIDE))[0] for vjp, weight in zip(gelu_vjps, fc2_all)]
    d_fc1_b = [jnp.sum(part, axis=(0, 1, 2)) for part in d_pre]
    d_pre = [part.astype(HALF) for part in d_pre]
    grad_fc1 = product('gbtf,gbtd->fd', d_pre[1], h_two)
    grad_fc1, d_pre = tie((grad_fc1, d_pre))
    d_h_two = summed('gbtf,fd->gbtd', d_pre, fc1_all).astype(HALF)
    d_h_two, d_pre[0] = tie((d_h_two, d_pre[0]))
    grad_fc1 = product('gbtf,gbtd->fd', d_pre[0], h_two) + swap(grad_fc1)
    grad_fc1, d_h_two, hidden = tie((grad_fc1, d_h_two, hidden))
    d_fc1_w = scatter(grad_fc1, 0)
    d_x_ln, d_ln2_scale, d_ln2_bias = ln_two_vjp(d_h_two.astype(WIDE))
    d_x_one = (d_out_img.astype(WIDE) + d_x_ln).astype(HALF)
    d_out_b = jnp.sum(d_x_one, axis=(0, 1, 2), dtype=WIDE)
    grad_out = product('gbtn,gbtd->nd', context[1], d_x_one)
    grad_out, d_x_one = tie((grad_out, d_x_one))
    d_context = [product('gbtd,nd->gbtn', d_x_one, weight).astype(HALF) for weight in out_all]
    d_context, context[0] = tie((d_context, context[0]))
    grad_out = product('gbtn,gbtd->nd', context[0], d_x_one) + swap(grad_out)
    grad_out, d_context, hidden = tie((grad_out, d_context, hidden))
    d_out_w = scatter(grad_out, 0)
    x_two = (x_one_f + (summed('gbtf,fd->gbtd', hidden, fc2_all) + fc2_b.astype(WIDE))).astype(HALF)
    x_two, d_context, d_fc2_w = tie((x_two, d_context, d_fc2_w))
    x_two = lax.all_to_all(x_two, 'tp', 0, 0, tiled=True).reshape(d_out.shape)
    d_qkv = [attention_backward(*args, heads_half, scale) for args in zip(qkv, d_context)]
    grad_qkv = product('sgbtn,gbtd->snd', d_qkv[1], h_one)
    grad_qkv, d_qkv = tie((grad_qkv, d_qkv))
    d_h_one = summed('sgbtn,snd->gbtd', d_qkv, qkv_all).astype(HALF)
    d_h_one, d_qkv = tie((d_h_one, d_qkv))
    grad_qkv = product('sgbtn,gbtd->snd', d_qkv[0], h_one) + swap(grad_qkv)
    grad_qkv, d_h_one = tie((grad_qkv, d_h_one))
    d_qkv_w = scatter(grad_qkv, 1)
    d_qkv_b = [jnp.sum(part, axis=(1, 2, 3), dtype=WIDE) for part in d_qkv]
    d_emb_ln, d_ln1_scale, d_ln1_bias = ln_one_vjp(d_h_one.astype(WIDE))
    d_emb = (d_x_one.astype(WIDE) + d_emb_ln).astype(HALF)
    d_emb, d_fc1_w = tie((d_emb, d_fc1_w))
    d_pos = jnp.sum(d_emb, axis=1, dtype=WIDE)
    d_patch_b = jnp.sum(d_emb, axis=(0, 1, 2), dtype=WIDE)
    d_patch_w = product('gbtp,gbtd->pd', patches_img, d_emb)

    shared = jnp.concatenate([d_patch_w, jnp.stack([d_patch_b, d_ln1_scale, d_ln2_scale, d_ln1_bias, d_ln2_bias, d_out_b, d_fc2_b])])
    shared_rows = shared.shape[0]
    shared = pad_rows(shared, round_up(shared_rows, 16 * size)).reshape(size, -1, dim)
    biases = [jnp.concatenate([fc1_part.reshape(size // 2, -1), qkv_part.reshape(3, size // 2, -1).transpose(1, 0, 2).reshape(size // 2, -1)], axis=1)
              for fc1_part, qkv_part in zip(d_fc1_b, d_qkv_b)]
    biases = jnp.where(core == 0, jnp.stack(biases, axis=1), jnp.stack(biases[::-1], axis=1)).reshape(size, 1, -1)
    biases = jnp.pad(biases, ((0, 0), (0, 7), (0, dim - biases.shape[2])))
    small = jnp.concatenate([d_pos, shared, biases], axis=1)
    small, x_two, d_out_w, d_qkv_w = tie((small, x_two, d_out_w, d_qkv_w))
    small = lax.psum_scatter(small, 'tp', scatter_dimension=0, tiled=True)[0]
    d_pos = small[:pos_rows].astype(HALF)
    d_fc1_b = small[-8, :cols_here]
    d_qkv_b = small[-8, cols_pad:cols_pad + 3 * head_rows].reshape(3, heads_here, width)
    shared = lax.all_gather(small[pos_rows:-8].astype(HALF), 'tp', axis=0, tiled=True)
    patch_rows = patch_w.shape[0]
    rest = shared[patch_rows:shared_rows]

    d_qkv_w = d_qkv_w.astype(HALF).reshape(3, heads_here, width, dim).transpose(0, 3, 1, 2)
    d_out_w = d_out_w.astype(HALF).reshape(heads_here, width, dim)
    d_fc1_w = d_fc1_w[:cols_here].astype(HALF).T
    d_fc2_w = d_fc2_w[:cols_here].astype(HALF)
    return (x_two, shared[:patch_rows], rest[0], d_pos, rest[1:3], rest[3:5], d_qkv_w, d_qkv_b.astype(HALF), d_out_w, rest[5], d_fc1_w, d_fc1_b.astype(HALF), d_fc2_w, rest[6])


def solution(mesh):
    in_specs = (P('dp', 'tp', None), P(), P(), P('tp', None), P(), P(), P(None, None, 'tp', None), P(None, 'tp', None), P('tp', None, None), P(), P(None, 'tp'), P('tp'), P('tp', None), P(), P('dp', 'tp', None))
    out_specs = (P('dp', 'tp', None), P('dp', None), P('dp'), P(('dp', 'tp'), None), P('dp', None), P('dp', None), P('dp', None, 'tp', None), P('dp', 'tp', None), P(('dp', 'tp'), None, None), P('dp'), P('dp', 'tp'), P(('dp', 'tp')), P(('dp', 'tp'), None), P('dp'))
    return jax.shard_map(group_step, mesh=mesh, in_specs=in_specs, out_specs=out_specs, check_vma=False)
```

```python
import functools

import jax
import jax.numpy as jnp
from jax import lax
from jax.experimental import pallas as pl
from jax.experimental.pallas import tpu as pltpu
from jax.sharding import PartitionSpec as P

LN_EPS = 1e-6
WIDE = jnp.float32
HALF = jnp.bfloat16


def layer_norm(x_val, scale_f, bias_f):
    row_mean = jnp.mean(x_val, axis=-1, keepdims=True)
    centered = x_val - row_mean
    row_var = jnp.mean(centered * centered, axis=-1, keepdims=True)
    return centered * lax.rsqrt(row_var + LN_EPS) * scale_f + bias_f


def gelu_tanh(pre_act):
    return jax.nn.gelu(pre_act, approximate=True)


def dot(a_val, b_val, contract):
    return lax.dot_general(a_val, b_val, ((contract[0], contract[1]), ((), ())), preferred_element_type=WIDE)


def attention_forward_kernel(heads, scale, qkv_ref, out_ref):
    width = qkv_ref.shape[-1] // heads
    for head in range(heads):
        cols = slice(head * width, (head + 1) * width)
        query, keys, values = (qkv_ref[part, :, 0, :, cols].reshape(-1, width) for part in range(3))
        scores = dot(keys, query, ((1,), (1,))) * scale
        scores = jnp.exp(scores - jnp.max(scores, axis=0, keepdims=True))
        probs = scores * (1.0 / jnp.sum(scores, axis=0, keepdims=True))
        context = dot(values, probs.astype(HALF), ((0,), (0,))).T.astype(HALF)
        out_ref[:, 0, :, cols] = context.reshape(out_ref.shape[0], -1, width)


def attention_backward_kernel(heads, scale, qkv_ref, d_ref, out_ref):
    width = qkv_ref.shape[-1] // heads
    for head in range(heads):
        cols = slice(head * width, (head + 1) * width)
        query, keys, values = (qkv_ref[part, :, 0, :, cols].reshape(-1, width) for part in range(3))
        d_context = d_ref[:, 0, :, cols].reshape(-1, width)
        scores = dot(keys, query, ((1,), (1,))) * scale
        scores = jnp.exp(scores - jnp.max(scores, axis=0, keepdims=True))
        probs = scores * (1.0 / jnp.sum(scores, axis=0, keepdims=True))
        d_probs = dot(values, d_context, ((1,), (1,))).astype(HALF).astype(WIDE)
        d_scores = probs * (d_probs - jnp.sum(d_probs * probs, axis=0, keepdims=True))
        d_scores = (d_scores * scale).astype(HALF)
        d_values = dot(probs.astype(HALF), d_context, ((1,), (0,))).astype(HALF)
        d_keys = dot(d_scores, query, ((1,), (0,))).astype(HALF)
        d_query = dot(keys, d_scores, ((0,), (0,))).T.astype(HALF)
        for part, grad in enumerate((d_query, d_keys, d_values)):
            out_ref[part, :, 0, :, cols] = grad.reshape(out_ref.shape[1], -1, width)


def attention_cost(images, heads, tokens, width, dots):
    return pl.CostEstimate(
        flops=2 * dots * images * heads * tokens * tokens * width,
        bytes_accessed=2 * (dots + 2) * images * heads * tokens * width,
        transcendentals=images * heads * tokens * tokens)


def attention_forward(qkv, heads, scale):
    _, blocks, images, rows, dim = qkv.shape
    return pl.pallas_call(
        functools.partial(attention_forward_kernel, heads, scale),
        out_shape=jax.ShapeDtypeStruct((blocks, images, rows, dim), HALF),
        grid=(images,),
        in_specs=[pl.BlockSpec((3, blocks, 1, rows, dim), lambda i: (0, 0, i, 0, 0))],
        out_specs=pl.BlockSpec((blocks, 1, rows, dim), lambda i: (0, i, 0, 0)),
        cost_estimate=attention_cost(images, heads, blocks * rows, dim // heads, 2),
        name='attention_forward',
    )(qkv)


def attention_backward(qkv, d_context, heads, scale):
    _, blocks, images, rows, dim = qkv.shape
    return pl.pallas_call(
        functools.partial(attention_backward_kernel, heads, scale),
        out_shape=jax.ShapeDtypeStruct(qkv.shape, HALF),
        grid=(images,),
        in_specs=[pl.BlockSpec((3, blocks, 1, rows, dim), lambda i: (0, 0, i, 0, 0)),
                  pl.BlockSpec((blocks, 1, rows, dim), lambda i: (0, i, 0, 0))],
        out_specs=pl.BlockSpec((3, blocks, 1, rows, dim), lambda i: (0, 0, i, 0, 0)),
        cost_estimate=attention_cost(images, heads, blocks * rows, dim // heads, 5),
        name='attention_backward',
    )(qkv, d_context)


def round_up(value, step):
    return (value + step - 1) // step * step


def pad_rows(x_val, rows):
    return jnp.pad(x_val, ((0, rows - x_val.shape[0]), (0, 0)))


def group_step(patches, patch_w, patch_b, pos_emb, ln_scale, ln_bias, qkv_w, qkv_b, out_w, out_b, fc1_w, fc1_b, fc2_w, fc2_b, d_out):
    size = lax.axis_size('tp')
    core = lax.rem(lax.axis_index('tp'), 2)
    same_core = [list(range(start, size, 2)) for start in range(2)]
    partner = [(index, index ^ 1) for index in range(size)]
    dim = patch_w.shape[1]
    heads_here, width = qkv_w.shape[2:]
    heads_half = heads_here * size // 2
    head_rows = heads_here * width
    scale = width ** -0.5
    cols_here = fc1_w.shape[1]
    cols_pad = round_up(cols_here, 32)
    ln_scale_f = ln_scale.astype(WIDE)
    ln_bias_f = ln_bias.astype(WIDE)
    tie = lax.optimization_barrier

    def images_of(x_val):
        x_val = x_val.reshape(size, -1, *x_val.shape[1:])
        return lax.all_to_all(x_val, 'tp', 0, 0, tiled=True)

    def gather(x_val, axis):
        return lax.all_gather(x_val, 'tp', axis=axis, tiled=True, axis_index_groups=same_core)

    def swap(x_val):
        return lax.ppermute(x_val, 'tp', partner)

    def scatter(x_val, axis):
        return lax.psum_scatter(x_val, 'tp', scatter_dimension=axis, tiled=True, axis_index_groups=same_core)

    def halves_of(table):
        table = table.reshape(size // 2, 2, *table.shape[1:])
        return [lax.dynamic_index_in_dim(table, index, 1, keepdims=False) for index in (core, 1 - core)]

    def product(spec, a_val, b_val):
        return jnp.einsum(spec, a_val, b_val, preferred_element_type=WIDE)

    def summed(spec, a_pair, b_pair):
        return product(spec, a_pair[0], b_pair[0]) + product(spec, a_pair[1], b_pair[1])

    pos_rows = pos_emb.shape[0]
    biases = jnp.concatenate([qkv_b.reshape(-1), fc1_b])
    biases = jnp.pad(biases, (0, dim - biases.shape[0]))[None]
    tables = pad_rows(jnp.concatenate([pos_emb, biases]), round_up(pos_rows + 1, 16))
    patches_img = images_of(patches)
    tables = lax.all_gather(tables, 'tp', axis=0)
    pos_all = tables[:, :pos_rows]
    qkv_b_all = [part.reshape(-1, 3, head_rows).transpose(1, 0, 2).reshape(3, 1, 1, 1, -1).astype(WIDE)
                 for part in halves_of(tables[:, pos_rows, :3 * head_rows])]
    fc1_b_all = [jnp.pad(part, ((0, 0), (0, cols_pad - cols_here))).reshape(-1).astype(WIDE)
                 for part in halves_of(tables[:, pos_rows, 3 * head_rows:3 * head_rows + cols_here])]
    attention_rows = jnp.concatenate([qkv_w.transpose(0, 2, 3, 1).reshape(3, head_rows, dim), out_w.reshape(1, head_rows, dim)])
    attention_own = gather(attention_rows, 1)
    fc1_own = gather(pad_rows(fc1_w.T, cols_pad), 0)
    d_out_img = images_of(d_out)
    fc2_own = gather(pad_rows(fc2_w, cols_pad), 0)

    emb = product('gbtp,pd->gbtd', patches_img, patch_w)
    emb_f = (emb + patch_b.astype(WIDE) + pos_all[:, None].astype(WIDE)).astype(HALF).astype(WIDE)
    h_one_f, ln_one_vjp = jax.vjp(layer_norm, emb_f, ln_scale_f[0], ln_bias_f[0])
    h_one = h_one_f.astype(HALF)
    attention_own, h_one = tie((attention_own, h_one))
    attention_all = [attention_own, swap(attention_own)]
    qkv_all = [part[:3] for part in attention_all]
    out_all = [part[3] for part in attention_all]
    qkv = [(product('gbtd,snd->sgbtn', h_one, weight) + bias).astype(HALF) for weight, bias in zip(qkv_all, qkv_b_all)]
    context = [attention_forward(part, heads_half, scale) for part in qkv]
    attn_out = summed('gbtn,nd->gbtd', context, out_all)
    x_one_f = (emb_f + (attn_out + out_b.astype(WIDE))).astype(HALF).astype(WIDE)
    h_two_f, ln_two_vjp = jax.vjp(layer_norm, x_one_f, ln_scale_f[1], ln_bias_f[1])
    h_two = h_two_f.astype(HALF)
    fc1_own, h_two, d_out_img = tie((fc1_own, h_two, d_out_img))
    fc1_all = [fc1_own, swap(fc1_own)]
    hidden, gelu_vjps = [], []
    for weight, bias in zip(fc1_all, fc1_b_all):
        hidden_f, gelu_vjp = jax.vjp(gelu_tanh, product('gbtd,fd->gbtf', h_two, weight) + bias)
        hidden.append(hidden_f.astype(HALF))
        gelu_vjps.append(gelu_vjp)


    d_fc2_b = jnp.sum(d_out.astype(WIDE), axis=(0, 1))
    grad_fc2 = product('gbtf,gbtd->fd', hidden[1], d_out_img)
    grad_fc2, hidden[0] = tie((grad_fc2, hidden[0]))
    grad_fc2 = product('gbtf,gbtd->fd', hidden[0], d_out_img) + swap(grad_fc2)
    grad_fc2, d_out_img, fc2_own, hidden = tie((grad_fc2, d_out_img, fc2_own, hidden))
    fc2_all = [fc2_own, swap(fc2_own)]
    d_fc2_w = scatter(grad_fc2, 0)
    d_pre = [vjp(product('gbtd,fd->gbtf', d_out_img, weight).astype(HALF).astype(WIDE))[0] for vjp, weight in zip(gelu_vjps, fc2_all)]
    d_fc1_b = [jnp.sum(part, axis=(0, 1, 2)) for part in d_pre]
    d_pre = [part.astype(HALF) for part in d_pre]
    grad_fc1 = product('gbtf,gbtd->fd', d_pre[1], h_two)
    grad_fc1, d_pre = tie((grad_fc1, d_pre))
    d_h_two = summed('gbtf,fd->gbtd', d_pre, fc1_all).astype(HALF)
    d_h_two, d_pre[0] = tie((d_h_two, d_pre[0]))
    grad_fc1 = product('gbtf,gbtd->fd', d_pre[0], h_two) + swap(grad_fc1)
    grad_fc1, d_h_two, hidden = tie((grad_fc1, d_h_two, hidden))
    d_fc1_w = scatter(grad_fc1, 0)
    d_x_ln, d_ln2_scale, d_ln2_bias = ln_two_vjp(d_h_two.astype(WIDE))
    d_x_one = (d_out_img.astype(WIDE) + d_x_ln).astype(HALF)
    d_out_b = jnp.sum(d_x_one, axis=(0, 1, 2), dtype=WIDE)
    grad_out = product('gbtn,gbtd->nd', context[1], d_x_one)
    grad_out, d_x_one = tie((grad_out, d_x_one))
    d_context = [product('gbtd,nd->gbtn', d_x_one, weight).astype(HALF) for weight in out_all]
    d_context, context[0] = tie((d_context, context[0]))
    grad_out = product('gbtn,gbtd->nd', context[0], d_x_one) + swap(grad_out)
    grad_out, d_context, hidden = tie((grad_out, d_context, hidden))
    d_out_w = scatter(grad_out, 0)
    x_two = (x_one_f + (summed('gbtf,fd->gbtd', hidden, fc2_all) + fc2_b.astype(WIDE))).astype(HALF)
    x_two, d_context, d_fc2_w = tie((x_two, d_context, d_fc2_w))
    x_two = lax.all_to_all(x_two, 'tp', 0, 0, tiled=True).reshape(d_out.shape)
    d_qkv = [attention_backward(*args, heads_half, scale) for args in zip(qkv, d_context)]
    grad_qkv = product('sgbtn,gbtd->snd', d_qkv[1], h_one)
    grad_qkv, d_qkv = tie((grad_qkv, d_qkv))
    d_h_one = summed('sgbtn,snd->gbtd', d_qkv, qkv_all).astype(HALF)
    d_h_one, d_qkv = tie((d_h_one, d_qkv))
    grad_qkv = product('sgbtn,gbtd->snd', d_qkv[0], h_one) + swap(grad_qkv)
    grad_qkv, d_h_one = tie((grad_qkv, d_h_one))
    d_qkv_w = scatter(grad_qkv, 1)
    d_qkv_b = [jnp.sum(part, axis=(1, 2, 3), dtype=WIDE) for part in d_qkv]
    d_emb_ln, d_ln1_scale, d_ln1_bias = ln_one_vjp(d_h_one.astype(WIDE))
    d_emb = (d_x_one.astype(WIDE) + d_emb_ln).astype(HALF)
    d_emb, d_fc1_w = tie((d_emb, d_fc1_w))
    d_pos = jnp.sum(d_emb, axis=1, dtype=WIDE)
    d_patch_b = jnp.sum(d_emb, axis=(0, 1, 2), dtype=WIDE)
    d_patch_w = product('gbtp,gbtd->pd', patches_img, d_emb)

    d_patch_w, d_out_w, x_two = tie((d_patch_w, d_out_w, x_two))
    biases = [jnp.concatenate([fc1_part.reshape(size // 2, -1), qkv_part.reshape(3, size // 2, -1).transpose(1, 0, 2).reshape(size // 2, -1)], axis=1)
              for fc1_part, qkv_part in zip(d_fc1_b, d_qkv_b)]
    biases = jnp.where(core == 0, jnp.stack(biases, axis=1), jnp.stack(biases[::-1], axis=1)).reshape(size, -1)
    d_ln_scale = jnp.stack([d_ln1_scale, d_ln2_scale])
    d_ln_bias = jnp.stack([d_ln1_bias, d_ln2_bias])
    small = (d_patch_w, d_patch_b, d_ln_scale, d_ln_bias, d_out_b, d_fc2_b, d_pos, biases)
    small = [part.astype(HALF) for part in lax.psum(small, 'tp')]
    d_patch_w, d_patch_b, d_ln_scale, d_ln_bias, d_out_b, d_fc2_b, d_pos, biases = small
    d_pos, biases = [lax.dynamic_index_in_dim(part, lax.axis_index('tp'), 0, keepdims=False) for part in (d_pos, biases)]
    d_fc1_b = biases[:cols_here]
    d_qkv_b = biases[cols_pad:].reshape(3, heads_here, width)

    d_qkv_w = d_qkv_w.astype(HALF).reshape(3, heads_here, width, dim).transpose(0, 3, 1, 2)
    d_out_w = d_out_w.astype(HALF).reshape(heads_here, width, dim)
    d_fc1_w = d_fc1_w[:cols_here].astype(HALF).T
    d_fc2_w = d_fc2_w[:cols_here].astype(HALF)
    return (x_two, d_patch_w, d_patch_b, d_pos, d_ln_scale, d_ln_bias, d_qkv_w, d_qkv_b, d_out_w, d_out_b, d_fc1_w, d_fc1_b, d_fc2_w, d_fc2_b)


def solution(mesh):
    in_specs = (P('dp', 'tp', None), P(), P(), P('tp', None), P(), P(), P(None, None, 'tp', None), P(None, 'tp', None), P('tp', None, None), P(), P(None, 'tp'), P('tp'), P('tp', None), P(), P('dp', 'tp', None))
    out_specs = (P('dp', 'tp', None), P('dp', None), P('dp'), P(('dp', 'tp'), None), P('dp', None), P('dp', None), P('dp', None, 'tp', None), P('dp', 'tp', None), P(('dp', 'tp'), None, None), P('dp'), P('dp', 'tp'), P(('dp', 'tp')), P(('dp', 'tp'), None), P('dp'))
    return jax.shard_map(group_step, mesh=mesh, in_specs=in_specs, out_specs=out_specs, check_vma=False)
```

```python
import functools

import jax
import jax.numpy as jnp
from jax import lax
from jax.experimental import pallas as pl
from jax.experimental.pallas import tpu as pltpu
from jax.sharding import PartitionSpec as P

LN_EPS = 1e-6
WIDE = jnp.float32
HALF = jnp.bfloat16


def layer_norm(x_val, scale_f, bias_f):
    row_mean = jnp.mean(x_val, axis=-1, keepdims=True)
    centered = x_val - row_mean
    row_var = jnp.mean(centered * centered, axis=-1, keepdims=True)
    return centered * lax.rsqrt(row_var + LN_EPS) * scale_f + bias_f


def gelu_tanh(pre_act):
    return jax.nn.gelu(pre_act, approximate=True)


def dot(a_val, b_val, contract):
    return lax.dot_general(a_val, b_val, ((contract[0], contract[1]), ((), ())), preferred_element_type=WIDE)


def attention_forward_kernel(heads, scale, qkv_ref, out_ref):
    width = qkv_ref.shape[-1] // heads
    for head in range(heads):
        cols = slice(head * width, (head + 1) * width)
        query, keys, values = (qkv_ref[part, :, 0, :, cols].reshape(-1, width) for part in range(3))
        scores = dot(keys, query, ((1,), (1,))) * scale
        scores = jnp.exp(scores - jnp.max(scores, axis=0, keepdims=True))
        probs = scores * (1.0 / jnp.sum(scores, axis=0, keepdims=True))
        context = dot(values, probs.astype(HALF), ((0,), (0,))).T.astype(HALF)
        out_ref[:, 0, :, cols] = context.reshape(out_ref.shape[0], -1, width)


def attention_backward_kernel(heads, scale, qkv_ref, d_ref, out_ref):
    width = qkv_ref.shape[-1] // heads
    for head in range(heads):
        cols = slice(head * width, (head + 1) * width)
        query, keys, values = (qkv_ref[part, :, 0, :, cols].reshape(-1, width) for part in range(3))
        d_context = d_ref[:, 0, :, cols].reshape(-1, width)
        scores = dot(keys, query, ((1,), (1,))) * scale
        scores = jnp.exp(scores - jnp.max(scores, axis=0, keepdims=True))
        probs = scores * (1.0 / jnp.sum(scores, axis=0, keepdims=True))
        d_probs = dot(values, d_context, ((1,), (1,))).astype(HALF).astype(WIDE)
        d_scores = probs * (d_probs - jnp.sum(d_probs * probs, axis=0, keepdims=True))
        d_scores = (d_scores * scale).astype(HALF)
        d_values = dot(probs.astype(HALF), d_context, ((1,), (0,))).astype(HALF)
        d_keys = dot(d_scores, query, ((1,), (0,))).astype(HALF)
        d_query = dot(keys, d_scores, ((0,), (0,))).T.astype(HALF)
        for part, grad in enumerate((d_query, d_keys, d_values)):
            out_ref[part, :, 0, :, cols] = grad.reshape(out_ref.shape[1], -1, width)


def attention_cost(images, heads, tokens, width, dots):
    return pl.CostEstimate(
        flops=2 * dots * images * heads * tokens * tokens * width,
        bytes_accessed=2 * (dots + 2) * images * heads * tokens * width,
        transcendentals=images * heads * tokens * tokens)


def attention_forward(qkv, heads, scale):
    _, blocks, images, rows, dim = qkv.shape
    return pl.pallas_call(
        functools.partial(attention_forward_kernel, heads, scale),
        out_shape=jax.ShapeDtypeStruct((blocks, images, rows, dim), HALF),
        grid=(images,),
        in_specs=[pl.BlockSpec((3, blocks, 1, rows, dim), lambda i: (0, 0, i, 0, 0))],
        out_specs=pl.BlockSpec((blocks, 1, rows, dim), lambda i: (0, i, 0, 0)),
        cost_estimate=attention_cost(images, heads, blocks * rows, dim // heads, 2),
        name='attention_forward',
    )(qkv)


def attention_backward(qkv, d_context, heads, scale):
    _, blocks, images, rows, dim = qkv.shape
    return pl.pallas_call(
        functools.partial(attention_backward_kernel, heads, scale),
        out_shape=jax.ShapeDtypeStruct(qkv.shape, HALF),
        grid=(images,),
        in_specs=[pl.BlockSpec((3, blocks, 1, rows, dim), lambda i: (0, 0, i, 0, 0)),
                  pl.BlockSpec((blocks, 1, rows, dim), lambda i: (0, i, 0, 0))],
        out_specs=pl.BlockSpec((3, blocks, 1, rows, dim), lambda i: (0, 0, i, 0, 0)),
        cost_estimate=attention_cost(images, heads, blocks * rows, dim // heads, 5),
        name='attention_backward',
    )(qkv, d_context)


def round_up(value, step):
    return (value + step - 1) // step * step


def pad_rows(x_val, rows):
    return jnp.pad(x_val, ((0, rows - x_val.shape[0]), (0, 0)))


def group_step(patches, patch_w, patch_b, pos_emb, ln_scale, ln_bias, qkv_w, qkv_b, out_w, out_b, fc1_w, fc1_b, fc2_w, fc2_b, d_out):
    size = lax.axis_size('tp')
    core = lax.rem(lax.axis_index('tp'), 2)
    same_core = [list(range(start, size, 2)) for start in range(2)]
    partner = [(index, index ^ 1) for index in range(size)]
    dim = patch_w.shape[1]
    heads_here, width = qkv_w.shape[2:]
    heads_half = heads_here * size // 2
    head_rows = heads_here * width
    scale = width ** -0.5
    cols_here = fc1_w.shape[1]
    cols_pad = round_up(cols_here, 32)
    ln_scale_f = ln_scale.astype(WIDE)
    ln_bias_f = ln_bias.astype(WIDE)
    tie = lax.optimization_barrier

    def images_of(x_val):
        x_val = x_val.reshape(size, -1, *x_val.shape[1:])
        return lax.all_to_all(x_val, 'tp', 0, 0, tiled=True)

    def gather(x_val, axis):
        return lax.all_gather(x_val, 'tp', axis=axis, tiled=True, axis_index_groups=same_core)

    def swap(x_val):
        return lax.ppermute(x_val, 'tp', partner)

    def scatter(x_val, axis):
        return lax.psum_scatter(x_val, 'tp', scatter_dimension=axis, tiled=True, axis_index_groups=same_core)

    def halves_of(table):
        table = table.reshape(size // 2, 2, *table.shape[1:])
        return [lax.dynamic_index_in_dim(table, index, 1, keepdims=False) for index in (core, 1 - core)]

    def product(spec, a_val, b_val):
        return jnp.einsum(spec, a_val, b_val, preferred_element_type=WIDE)

    def summed(spec, a_pair, b_pair):
        return product(spec, a_pair[0], b_pair[0]) + product(spec, a_pair[1], b_pair[1])

    def chip_product(spec, left, left_partner, right, right_partner):
        part = product(spec, left, right)
        part, left_partner = tie((part, left_partner))
        return part + product(spec, left_partner, right_partner)

    pos_rows = pos_emb.shape[0]
    biases = jnp.concatenate([qkv_b.reshape(-1), fc1_b])
    biases = jnp.pad(biases, (0, dim - biases.shape[0]))[None]
    tables = pad_rows(jnp.concatenate([pos_emb, biases]), round_up(pos_rows + 1, 16))
    patches_img = images_of(patches)
    tables = lax.all_gather(tables, 'tp', axis=0)
    pos_all = tables[:, :pos_rows]
    qkv_b_all = [part.reshape(-1, 3, head_rows).transpose(1, 0, 2).reshape(3, 1, 1, 1, -1).astype(WIDE)
                 for part in halves_of(tables[:, pos_rows, :3 * head_rows])]
    fc1_b_all = [jnp.pad(part, ((0, 0), (0, cols_pad - cols_here))).reshape(-1).astype(WIDE)
                 for part in halves_of(tables[:, pos_rows, 3 * head_rows:3 * head_rows + cols_here])]
    attention_rows = jnp.concatenate([qkv_w.transpose(0, 2, 3, 1).reshape(3, head_rows, dim), out_w.reshape(1, head_rows, dim)])
    attention_own = gather(attention_rows, 1)
    fc1_own = gather(pad_rows(fc1_w.T, cols_pad), 0)
    d_out_img = images_of(d_out)
    fc2_own = gather(pad_rows(fc2_w, cols_pad), 0)

    emb = product('gbtp,pd->gbtd', patches_img, patch_w)
    emb_f = (emb + patch_b.astype(WIDE) + pos_all[:, None].astype(WIDE)).astype(HALF).astype(WIDE)
    h_one_f, ln_one_vjp = jax.vjp(layer_norm, emb_f, ln_scale_f[0], ln_bias_f[0])
    h_one = h_one_f.astype(HALF)
    attention_own, h_one = tie((attention_own, h_one))
    attention_all = [attention_own, swap(attention_own)]
    qkv_all = [part[:3] for part in attention_all]
    out_all = [part[3] for part in attention_all]
    qkv = [(product('gbtd,snd->sgbtn', h_one, weight) + bias).astype(HALF) for weight, bias in zip(qkv_all, qkv_b_all)]
    h_one_partner = swap(h_one)
    context = [attention_forward(part, heads_half, scale) for part in qkv]
    attn_out = summed('gbtn,nd->gbtd', context, out_all)
    x_one_f = (emb_f + (attn_out + out_b.astype(WIDE))).astype(HALF).astype(WIDE)
    h_two_f, ln_two_vjp = jax.vjp(layer_norm, x_one_f, ln_scale_f[1], ln_bias_f[1])
    h_two = h_two_f.astype(HALF)
    d_out_img, x_one_f = tie((d_out_img, x_one_f))
    d_out_partner = swap(d_out_img)
    fc1_own, h_two, d_out_img, d_out_partner = tie((fc1_own, h_two, d_out_img, d_out_partner))
    h_two_partner = swap(h_two)
    fc1_all = [fc1_own, swap(fc1_own)]
    hidden, gelu_vjps, rows = [], [], h_two
    for weight, bias in zip(fc1_all, fc1_b_all):
        hidden_f, gelu_vjp = jax.vjp(gelu_tanh, product('gbtd,fd->gbtf', rows, weight) + bias)
        hidden_h, rows = tie((hidden_f.astype(HALF), rows))
        hidden.append(hidden_h)
        gelu_vjps.append(gelu_vjp)


    d_fc2_b = jnp.sum(d_out.astype(WIDE), axis=(0, 1))
    grad_fc2 = chip_product('gbtf,gbtd->fd', hidden[0], swap(hidden[1]), d_out_img, d_out_partner)
    grad_fc2, d_out_img, fc2_own, hidden = tie((grad_fc2, d_out_img, fc2_own, hidden))
    fc2_all = [fc2_own, swap(fc2_own)]
    d_fc2_w = scatter(grad_fc2, 0)
    d_pre, d_fc1_b, rows = [], [], d_out_img
    for gelu_vjp, weight in zip(gelu_vjps, fc2_all):
        part = gelu_vjp(product('gbtd,fd->gbtf', rows, weight).astype(HALF).astype(WIDE))[0]
        d_fc1_b.append(jnp.sum(part, axis=(0, 1, 2)))
        part, rows = tie((part.astype(HALF), rows))
        d_pre.append(part)
    d_h_two = summed('gbtf,fd->gbtd', d_pre, fc1_all).astype(HALF)
    d_pre_partner = swap(d_pre[1])
    d_h_two, d_pre, d_pre_partner = tie((d_h_two, d_pre, d_pre_partner))
    grad_fc1 = chip_product('gbtf,gbtd->fd', d_pre[0], d_pre_partner, h_two, h_two_partner)
    grad_fc1, d_h_two, hidden = tie((grad_fc1, d_h_two, hidden))
    d_fc1_w = scatter(grad_fc1, 0)
    d_x_ln, d_ln2_scale, d_ln2_bias = ln_two_vjp(d_h_two.astype(WIDE))
    d_x_one = (d_out_img.astype(WIDE) + d_x_ln).astype(HALF)
    d_out_b = jnp.sum(d_x_one, axis=(0, 1, 2), dtype=WIDE)
    d_context = [product('gbtd,nd->gbtn', d_x_one, weight).astype(HALF) for weight in out_all]
    d_x_partner, context_partner = swap(d_x_one), swap(context[1])
    d_context, d_fc2_w = tie((d_context, d_fc2_w))
    d_qkv = [attention_backward(*args, heads_half, scale) for args in zip(qkv[::-1], d_context[::-1])][::-1]
    d_x_partner, context_partner, d_qkv = tie((d_x_partner, context_partner, d_qkv))
    d_qkv_partner = swap(d_qkv[1])
    grad_out = chip_product('gbtn,gbtd->nd', context[0], context_partner, d_x_one, d_x_partner)
    grad_out, d_qkv, d_qkv_partner = tie((grad_out, d_qkv, d_qkv_partner))
    grad_qkv = chip_product('sgbtn,gbtd->snd', d_qkv[0], d_qkv_partner, h_one, h_one_partner)
    grad_qkv, grad_out, d_qkv, hidden = tie((grad_qkv, grad_out, d_qkv, hidden))
    grad_attention = scatter(jnp.concatenate([grad_qkv, grad_out[None]]), 1)
    d_h_one = summed('sgbtn,snd->gbtd', d_qkv, qkv_all).astype(HALF)
    d_qkv_b = [jnp.sum(part, axis=(1, 2, 3), dtype=WIDE) for part in d_qkv]
    x_two = (x_one_f + (summed('gbtf,fd->gbtd', hidden, fc2_all) + fc2_b.astype(WIDE))).astype(HALF)
    x_two = lax.all_to_all(x_two, 'tp', 0, 0, tiled=True).reshape(d_out.shape)
    d_emb_ln, d_ln1_scale, d_ln1_bias = ln_one_vjp(d_h_one.astype(WIDE))
    d_emb = (d_x_one.astype(WIDE) + d_emb_ln).astype(HALF)
    d_pos = jnp.sum(d_emb, axis=1, dtype=WIDE)
    d_patch_b = jnp.sum(d_emb, axis=(0, 1, 2), dtype=WIDE)
    d_patch_w = product('gbtp,gbtd->pd', patches_img, d_emb)

    d_fc1_w = d_fc1_w[:cols_here].astype(HALF).T
    d_patch_w, d_fc1_w, x_two = tie((d_patch_w, d_fc1_w, x_two))
    biases = [jnp.concatenate([fc1_part.reshape(size // 2, -1), qkv_part.reshape(3, size // 2, -1).transpose(1, 0, 2).reshape(size // 2, -1)], axis=1)
              for fc1_part, qkv_part in zip(d_fc1_b, d_qkv_b)]
    biases = jnp.where(core == 0, jnp.stack(biases, axis=1), jnp.stack(biases[::-1], axis=1)).reshape(size, -1)
    d_ln_scale = jnp.stack([d_ln1_scale, d_ln2_scale])
    d_ln_bias = jnp.stack([d_ln1_bias, d_ln2_bias])
    small = (d_patch_w, d_patch_b, d_ln_scale, d_ln_bias, d_out_b, d_fc2_b, d_pos, biases)
    small = [part.astype(HALF) for part in lax.psum(small, 'tp')]
    d_patch_w, d_patch_b, d_ln_scale, d_ln_bias, d_out_b, d_fc2_b, d_pos, biases = small
    d_pos, biases = [lax.dynamic_index_in_dim(part, lax.axis_index('tp'), 0, keepdims=False) for part in (d_pos, biases)]
    d_fc1_b = biases[:cols_here]
    d_qkv_b = biases[cols_pad:].reshape(3, heads_here, width)

    d_qkv_w = grad_attention[:3].astype(HALF).reshape(3, heads_here, width, dim).transpose(0, 3, 1, 2)
    d_out_w = grad_attention[3].astype(HALF).reshape(heads_here, width, dim)
    d_fc2_w = d_fc2_w[:cols_here].astype(HALF)
    return (x_two, d_patch_w, d_patch_b, d_pos, d_ln_scale, d_ln_bias, d_qkv_w, d_qkv_b, d_out_w, d_out_b, d_fc1_w, d_fc1_b, d_fc2_w, d_fc2_b)


def solution(mesh):
    in_specs = (P('dp', 'tp', None), P(), P(), P('tp', None), P(), P(), P(None, None, 'tp', None), P(None, 'tp', None), P('tp', None, None), P(), P(None, 'tp'), P('tp'), P('tp', None), P(), P('dp', 'tp', None))
    out_specs = (P('dp', 'tp', None), P('dp', None), P('dp'), P(('dp', 'tp'), None), P('dp', None), P('dp', None), P('dp', None, 'tp', None), P('dp', 'tp', None), P(('dp', 'tp'), None, None), P('dp'), P('dp', 'tp'), P(('dp', 'tp')), P(('dp', 'tp'), None), P('dp'))
    return jax.shard_map(group_step, mesh=mesh, in_specs=in_specs, out_specs=out_specs, check_vma=False)
```

```python
import functools

import jax
import jax.numpy as jnp
from jax import lax
from jax.experimental import pallas as pl
from jax.experimental.pallas import tpu as pltpu
from jax.sharding import PartitionSpec as P

LN_EPS = 1e-6
WIDE = jnp.float32
HALF = jnp.bfloat16


def layer_norm(x_val, scale_f, bias_f):
    row_mean = jnp.mean(x_val, axis=-1, keepdims=True)
    centered = x_val - row_mean
    row_var = jnp.mean(centered * centered, axis=-1, keepdims=True)
    return centered * lax.rsqrt(row_var + LN_EPS) * scale_f + bias_f


def gelu_tanh(pre_act):
    return jax.nn.gelu(pre_act, approximate=True)


def dot(a_val, b_val, contract):
    return lax.dot_general(a_val, b_val, ((contract[0], contract[1]), ((), ())), preferred_element_type=WIDE)


def attention_forward_kernel(heads, scale, qkv_ref, out_ref):
    width = qkv_ref.shape[-1] // heads
    for head in range(heads):
        cols = slice(head * width, (head + 1) * width)
        query, keys, values = (qkv_ref[part, :, 0, :, cols].reshape(-1, width) for part in range(3))
        scores = dot(keys, query, ((1,), (1,))) * scale
        scores = jnp.exp(scores - jnp.max(scores, axis=0, keepdims=True))
        probs = scores * (1.0 / jnp.sum(scores, axis=0, keepdims=True))
        context = dot(values, probs.astype(HALF), ((0,), (0,))).T.astype(HALF)
        out_ref[:, 0, :, cols] = context.reshape(out_ref.shape[0], -1, width)


def attention_backward_kernel(heads, scale, qkv_ref, d_ref, out_ref):
    width = qkv_ref.shape[-1] // heads
    for head in range(heads):
        cols = slice(head * width, (head + 1) * width)
        query, keys, values = (qkv_ref[part, :, 0, :, cols].reshape(-1, width) for part in range(3))
        d_context = d_ref[:, 0, :, cols].reshape(-1, width)
        scores = dot(keys, query, ((1,), (1,))) * scale
        scores = jnp.exp(scores - jnp.max(scores, axis=0, keepdims=True))
        probs = scores * (1.0 / jnp.sum(scores, axis=0, keepdims=True))
        d_probs = dot(values, d_context, ((1,), (1,))).astype(HALF).astype(WIDE)
        d_scores = probs * (d_probs - jnp.sum(d_probs * probs, axis=0, keepdims=True))
        d_scores = (d_scores * scale).astype(HALF)
        d_values = dot(probs.astype(HALF), d_context, ((1,), (0,))).astype(HALF)
        d_keys = dot(d_scores, query, ((1,), (0,))).astype(HALF)
        d_query = dot(keys, d_scores, ((0,), (0,))).T.astype(HALF)
        for part, grad in enumerate((d_query, d_keys, d_values)):
            out_ref[part, :, 0, :, cols] = grad.reshape(out_ref.shape[1], -1, width)


def attention_cost(images, heads, tokens, width, dots):
    return pl.CostEstimate(
        flops=2 * dots * images * heads * tokens * tokens * width,
        bytes_accessed=2 * (dots + 2) * images * heads * tokens * width,
        transcendentals=images * heads * tokens * tokens)


def attention_forward(qkv, heads, scale):
    _, blocks, images, rows, dim = qkv.shape
    return pl.pallas_call(
        functools.partial(attention_forward_kernel, heads, scale),
        out_shape=jax.ShapeDtypeStruct((blocks, images, rows, dim), HALF),
        grid=(images,),
        in_specs=[pl.BlockSpec((3, blocks, 1, rows, dim), lambda i: (0, 0, i, 0, 0))],
        out_specs=pl.BlockSpec((blocks, 1, rows, dim), lambda i: (0, i, 0, 0)),
        cost_estimate=attention_cost(images, heads, blocks * rows, dim // heads, 2),
        name='attention_forward',
    )(qkv)


def attention_backward(qkv, d_context, heads, scale):
    _, blocks, images, rows, dim = qkv.shape
    return pl.pallas_call(
        functools.partial(attention_backward_kernel, heads, scale),
        out_shape=jax.ShapeDtypeStruct(qkv.shape, HALF),
        grid=(images,),
        in_specs=[pl.BlockSpec((3, blocks, 1, rows, dim), lambda i: (0, 0, i, 0, 0)),
                  pl.BlockSpec((blocks, 1, rows, dim), lambda i: (0, i, 0, 0))],
        out_specs=pl.BlockSpec((3, blocks, 1, rows, dim), lambda i: (0, 0, i, 0, 0)),
        cost_estimate=attention_cost(images, heads, blocks * rows, dim // heads, 5),
        name='attention_backward',
    )(qkv, d_context)


def round_up(value, step):
    return (value + step - 1) // step * step


def pad_rows(x_val, rows):
    return jnp.pad(x_val, ((0, rows - x_val.shape[0]), (0, 0)))


def group_step(patches, patch_w, patch_b, pos_emb, ln_scale, ln_bias, qkv_w, qkv_b, out_w, out_b, fc1_w, fc1_b, fc2_w, fc2_b, d_out):
    size = lax.axis_size('tp')
    core = lax.rem(lax.axis_index('tp'), 2)
    same_core = [list(range(start, size, 2)) for start in range(2)]
    partner = [(index, index ^ 1) for index in range(size)]
    dim = patch_w.shape[1]
    heads_here, width = qkv_w.shape[2:]
    heads_half = heads_here * size // 2
    head_rows = heads_here * width
    scale = width ** -0.5
    cols_here = fc1_w.shape[1]
    cols_pad = round_up(cols_here, 32)
    ln_scale_f = ln_scale.astype(WIDE)
    ln_bias_f = ln_bias.astype(WIDE)
    tie = lax.optimization_barrier

    def images_of(x_val):
        x_val = x_val.reshape(size, -1, *x_val.shape[1:])
        return lax.all_to_all(x_val, 'tp', 0, 0, tiled=True)

    def gather(x_val, axis):
        return lax.all_gather(x_val, 'tp', axis=axis, tiled=True, axis_index_groups=same_core)

    def swap(x_val):
        return lax.ppermute(x_val, 'tp', partner)

    def scatter(x_val, axis):
        return lax.psum_scatter(x_val, 'tp', scatter_dimension=axis, tiled=True, axis_index_groups=same_core)

    def halves_of(table):
        table = table.reshape(size // 2, 2, *table.shape[1:])
        return [lax.dynamic_index_in_dim(table, index, 1, keepdims=False) for index in (core, 1 - core)]

    def product(spec, a_val, b_val):
        return jnp.einsum(spec, a_val, b_val, preferred_element_type=WIDE)

    def summed(spec, a_pair, b_pair):
        return product(spec, a_pair[0], b_pair[0]) + product(spec, a_pair[1], b_pair[1])

    def chip_product(spec, left, left_partner, right, right_partner):
        return product(spec, left_partner, right_partner) + tie(product(spec, left, right))

    pos_rows = pos_emb.shape[0]
    biases = jnp.concatenate([qkv_b.reshape(-1), fc1_b])
    biases = jnp.pad(biases, (0, dim - biases.shape[0]))[None]
    tables = pad_rows(jnp.concatenate([pos_emb, biases]), round_up(pos_rows + 1, 16))
    patches_img = images_of(patches)
    tables = lax.all_gather(tables, 'tp', axis=0)
    pos_all = tables[:, :pos_rows]
    qkv_b_all = [part.reshape(-1, 3, head_rows).transpose(1, 0, 2).reshape(3, 1, 1, 1, -1).astype(WIDE)
                 for part in halves_of(tables[:, pos_rows, :3 * head_rows])]
    fc1_b_all = [jnp.pad(part, ((0, 0), (0, cols_pad - cols_here))).reshape(-1).astype(WIDE)
                 for part in halves_of(tables[:, pos_rows, 3 * head_rows:3 * head_rows + cols_here])]
    attention_rows = jnp.concatenate([qkv_w.transpose(0, 2, 3, 1).reshape(3, head_rows, dim), out_w.reshape(1, head_rows, dim)])
    attention_own = gather(attention_rows, 1)
    fc1_own = gather(pad_rows(fc1_w.T, cols_pad), 0)
    d_out_img = images_of(d_out)
    fc2_own = gather(pad_rows(fc2_w, cols_pad), 0)

    emb = product('gbtp,pd->gbtd', patches_img, patch_w)
    emb_f = (emb + patch_b.astype(WIDE) + pos_all[:, None].astype(WIDE)).astype(HALF).astype(WIDE)
    h_one_f, ln_one_vjp = jax.vjp(layer_norm, emb_f, ln_scale_f[0], ln_bias_f[0])
    h_one = h_one_f.astype(HALF)
    attention_own, h_one = tie((attention_own, h_one))
    attention_all = [attention_own, swap(attention_own)]
    qkv_all = [part[:3] for part in attention_all]
    out_all = [part[3] for part in attention_all]
    qkv = [(product('gbtd,snd->sgbtn', h_one, weight) + bias).astype(HALF) for weight, bias in zip(qkv_all, qkv_b_all)]
    h_one_partner = swap(h_one)
    context = [attention_forward(part, heads_half, scale) for part in qkv]
    attn_out = summed('gbtn,nd->gbtd', context, out_all)
    x_one_f = (emb_f + (attn_out + out_b.astype(WIDE))).astype(HALF).astype(WIDE)
    h_two_f, ln_two_vjp = jax.vjp(layer_norm, x_one_f, ln_scale_f[1], ln_bias_f[1])
    h_two = h_two_f.astype(HALF)
    d_out_img, x_one_f = tie((d_out_img, x_one_f))
    d_out_partner = swap(d_out_img)
    fc1_own, h_two, d_out_img, d_out_partner = tie((fc1_own, h_two, d_out_img, d_out_partner))
    h_two_partner = swap(h_two)
    fc1_all = [fc1_own, swap(fc1_own)]
    hidden, gelu_vjps, rows = [], [], h_two
    for weight, bias in zip(fc1_all, fc1_b_all):
        hidden_f, gelu_vjp = jax.vjp(gelu_tanh, product('gbtd,fd->gbtf', rows, weight) + bias)
        hidden_h, rows = tie((hidden_f.astype(HALF), rows))
        hidden.append(hidden_h)
        gelu_vjps.append(gelu_vjp)


    d_fc2_b = jnp.sum(d_out.astype(WIDE), axis=(0, 1))
    grad_fc2 = chip_product('gbtf,gbtd->fd', hidden[0], swap(hidden[1]), d_out_img, d_out_partner)
    grad_fc2, d_out_img, fc2_own, hidden = tie((grad_fc2, d_out_img, fc2_own, hidden))
    fc2_all = [fc2_own, swap(fc2_own)]
    d_fc2_w = scatter(grad_fc2, 0)
    d_pre, d_fc1_b, rows = [], [], d_out_img
    for gelu_vjp, weight in zip(gelu_vjps, fc2_all):
        part = gelu_vjp(product('gbtd,fd->gbtf', rows, weight).astype(HALF).astype(WIDE))[0]
        d_fc1_b.append(jnp.sum(part, axis=(0, 1, 2)))
        part, rows = tie((part.astype(HALF), rows))
        d_pre.append(part)
    d_h_two = summed('gbtf,fd->gbtd', d_pre, fc1_all).astype(HALF)
    d_pre_partner = swap(d_pre[1])
    d_h_two, d_pre, d_pre_partner, hidden = tie((d_h_two, d_pre, d_pre_partner, hidden))
    x_two = (x_one_f + (summed('gbtf,fd->gbtd', hidden, fc2_all) + fc2_b.astype(WIDE))).astype(HALF)
    x_two, d_pre, d_pre_partner = tie((x_two, d_pre, d_pre_partner))
    x_two = lax.all_to_all(x_two, 'tp', 0, 0, tiled=True).reshape(d_out.shape)
    grad_fc1 = chip_product('gbtf,gbtd->fd', d_pre[0], d_pre_partner, h_two, h_two_partner)
    grad_fc1, d_h_two = tie((grad_fc1, d_h_two))
    d_fc1_w = scatter(grad_fc1, 0)
    d_x_ln, d_ln2_scale, d_ln2_bias = ln_two_vjp(d_h_two.astype(WIDE))
    d_x_one = (d_out_img.astype(WIDE) + d_x_ln).astype(HALF)
    d_out_b = jnp.sum(d_x_one, axis=(0, 1, 2), dtype=WIDE)
    d_context = [product('gbtd,nd->gbtn', d_x_one, weight).astype(HALF) for weight in out_all]
    d_x_partner, context_partner = swap(d_x_one), swap(context[1])
    d_context, d_fc2_w = tie((d_context, d_fc2_w))
    d_qkv = [attention_backward(*args, heads_half, scale) for args in zip(qkv[::-1], d_context[::-1])][::-1]
    d_x_partner, context_partner, d_qkv, x_two = tie((d_x_partner, context_partner, d_qkv, x_two))
    d_qkv_partner = swap(d_qkv[1])
    grad_out = chip_product('gbtn,gbtd->nd', context[0], context_partner, d_x_one, d_x_partner)
    grad_out, d_qkv, d_qkv_partner = tie((grad_out, d_qkv, d_qkv_partner))
    grad_qkv = chip_product('sgbtn,gbtd->snd', d_qkv[0], d_qkv_partner, h_one, h_one_partner)
    grad_qkv, grad_out, d_qkv = tie((grad_qkv, grad_out, d_qkv))
    grad_attention = scatter(jnp.concatenate([grad_qkv, grad_out[None]]), 1)
    d_h_one = summed('sgbtn,snd->gbtd', d_qkv, qkv_all).astype(HALF)
    d_qkv_b = [jnp.sum(part, axis=(1, 2, 3), dtype=WIDE) for part in d_qkv]
    d_emb_ln, d_ln1_scale, d_ln1_bias = ln_one_vjp(d_h_one.astype(WIDE))
    d_emb = (d_x_one.astype(WIDE) + d_emb_ln).astype(HALF)
    d_pos = jnp.sum(d_emb, axis=1, dtype=WIDE)
    d_patch_b = jnp.sum(d_emb, axis=(0, 1, 2), dtype=WIDE)
    d_patch_w = product('gbtp,gbtd->pd', patches_img, d_emb)

    d_fc1_w = d_fc1_w[:cols_here].astype(HALF).T
    d_patch_w, d_fc1_w = tie((d_patch_w, d_fc1_w))
    biases = [jnp.concatenate([fc1_part.reshape(size // 2, -1), qkv_part.reshape(3, size // 2, -1).transpose(1, 0, 2).reshape(size // 2, -1)], axis=1)
              for fc1_part, qkv_part in zip(d_fc1_b, d_qkv_b)]
    biases = jnp.where(core == 0, jnp.stack(biases, axis=1), jnp.stack(biases[::-1], axis=1)).reshape(size, -1)
    d_ln_scale = jnp.stack([d_ln1_scale, d_ln2_scale])
    d_ln_bias = jnp.stack([d_ln1_bias, d_ln2_bias])
    small = (d_patch_w, d_patch_b, d_ln_scale, d_ln_bias, d_out_b, d_fc2_b, d_pos, biases)
    small = [part.astype(HALF) for part in lax.psum(small, 'tp')]
    d_patch_w, d_patch_b, d_ln_scale, d_ln_bias, d_out_b, d_fc2_b, d_pos, biases = small
    d_pos, biases = [lax.dynamic_index_in_dim(part, lax.axis_index('tp'), 0, keepdims=False) for part in (d_pos, biases)]
    d_fc1_b = biases[:cols_here]
    d_qkv_b = biases[cols_pad:].reshape(3, heads_here, width)

    d_qkv_w = grad_attention[:3].astype(HALF).reshape(3, heads_here, width, dim).transpose(0, 3, 1, 2)
    d_out_w = grad_attention[3].astype(HALF).reshape(heads_here, width, dim)
    d_fc2_w = d_fc2_w[:cols_here].astype(HALF)
    return (x_two, d_patch_w, d_patch_b, d_pos, d_ln_scale, d_ln_bias, d_qkv_w, d_qkv_b, d_out_w, d_out_b, d_fc1_w, d_fc1_b, d_fc2_w, d_fc2_b)


def solution(mesh):
    in_specs = (P('dp', 'tp', None), P(), P(), P('tp', None), P(), P(), P(None, None, 'tp', None), P(None, 'tp', None), P('tp', None, None), P(), P(None, 'tp'), P('tp'), P('tp', None), P(), P('dp', 'tp', None))
    out_specs = (P('dp', 'tp', None), P('dp', None), P('dp'), P(('dp', 'tp'), None), P('dp', None), P('dp', None), P('dp', None, 'tp', None), P('dp', 'tp', None), P(('dp', 'tp'), None, None), P('dp'), P('dp', 'tp'), P(('dp', 'tp')), P(('dp', 'tp'), None), P('dp'))
    return jax.shard_map(group_step, mesh=mesh, in_specs=in_specs, out_specs=out_specs, check_vma=False)
```

```python
import functools

import jax
import jax.numpy as jnp
from jax import lax
from jax.experimental import pallas as pl
from jax.experimental.pallas import tpu as pltpu
from jax.sharding import PartitionSpec as P

LN_EPS = 1e-6
WIDE = jnp.float32
HALF = jnp.bfloat16


def layer_norm(x_val, scale_f, bias_f):
    row_mean = jnp.mean(x_val, axis=-1, keepdims=True)
    centered = x_val - row_mean
    row_var = jnp.mean(centered * centered, axis=-1, keepdims=True)
    return centered * lax.rsqrt(row_var + LN_EPS) * scale_f + bias_f


def gelu_tanh(pre_act):
    return jax.nn.gelu(pre_act, approximate=True)


def dot(a_val, b_val, contract):
    return lax.dot_general(a_val, b_val, ((contract[0], contract[1]), ((), ())), preferred_element_type=WIDE)


def attention_forward_kernel(heads, scale, qkv_ref, out_ref):
    width = qkv_ref.shape[-1] // heads
    for head in range(heads):
        cols = slice(head * width, (head + 1) * width)
        query, keys, values = (qkv_ref[part, :, 0, :, cols].reshape(-1, width) for part in range(3))
        scores = dot(keys, query, ((1,), (1,))) * scale
        scores = jnp.exp(scores - jnp.max(scores, axis=0, keepdims=True))
        probs = scores * (1.0 / jnp.sum(scores, axis=0, keepdims=True))
        context = dot(values, probs.astype(HALF), ((0,), (0,))).T.astype(HALF)
        out_ref[:, 0, :, cols] = context.reshape(out_ref.shape[0], -1, width)


def attention_backward_kernel(heads, scale, qkv_ref, d_ref, out_ref):
    width = qkv_ref.shape[-1] // heads
    for head in range(heads):
        cols = slice(head * width, (head + 1) * width)
        query, keys, values = (qkv_ref[part, :, 0, :, cols].reshape(-1, width) for part in range(3))
        d_context = d_ref[:, 0, :, cols].reshape(-1, width)
        scores = dot(keys, query, ((1,), (1,))) * scale
        scores = jnp.exp(scores - jnp.max(scores, axis=0, keepdims=True))
        probs = scores * (1.0 / jnp.sum(scores, axis=0, keepdims=True))
        d_probs = dot(values, d_context, ((1,), (1,))).astype(HALF).astype(WIDE)
        d_scores = probs * (d_probs - jnp.sum(d_probs * probs, axis=0, keepdims=True))
        d_scores = (d_scores * scale).astype(HALF)
        d_values = dot(probs.astype(HALF), d_context, ((1,), (0,))).astype(HALF)
        d_keys = dot(d_scores, query, ((1,), (0,))).astype(HALF)
        d_query = dot(keys, d_scores, ((0,), (0,))).T.astype(HALF)
        for part, grad in enumerate((d_query, d_keys, d_values)):
            out_ref[part, :, 0, :, cols] = grad.reshape(out_ref.shape[1], -1, width)


def attention_cost(images, heads, tokens, width, dots):
    return pl.CostEstimate(
        flops=2 * dots * images * heads * tokens * tokens * width,
        bytes_accessed=2 * (dots + 2) * images * heads * tokens * width,
        transcendentals=images * heads * tokens * tokens)


def attention_forward(qkv, heads, scale):
    _, blocks, images, rows, dim = qkv.shape
    return pl.pallas_call(
        functools.partial(attention_forward_kernel, heads, scale),
        out_shape=jax.ShapeDtypeStruct((blocks, images, rows, dim), HALF),
        grid=(images,),
        in_specs=[pl.BlockSpec((3, blocks, 1, rows, dim), lambda i: (0, 0, i, 0, 0))],
        out_specs=pl.BlockSpec((blocks, 1, rows, dim), lambda i: (0, i, 0, 0)),
        cost_estimate=attention_cost(images, heads, blocks * rows, dim // heads, 2),
        name='attention_forward',
    )(qkv)


def attention_backward(qkv, d_context, heads, scale):
    _, blocks, images, rows, dim = qkv.shape
    return pl.pallas_call(
        functools.partial(attention_backward_kernel, heads, scale),
        out_shape=jax.ShapeDtypeStruct(qkv.shape, HALF),
        grid=(images,),
        in_specs=[pl.BlockSpec((3, blocks, 1, rows, dim), lambda i: (0, 0, i, 0, 0)),
                  pl.BlockSpec((blocks, 1, rows, dim), lambda i: (0, i, 0, 0))],
        out_specs=pl.BlockSpec((3, blocks, 1, rows, dim), lambda i: (0, 0, i, 0, 0)),
        cost_estimate=attention_cost(images, heads, blocks * rows, dim // heads, 5),
        name='attention_backward',
    )(qkv, d_context)


def round_up(value, step):
    return (value + step - 1) // step * step


def pad_rows(x_val, rows):
    return jnp.pad(x_val, ((0, rows - x_val.shape[0]), (0, 0)))


def group_step(patches, patch_w, patch_b, pos_emb, ln_scale, ln_bias, qkv_w, qkv_b, out_w, out_b, fc1_w, fc1_b, fc2_w, fc2_b, d_out):
    size = lax.axis_size('tp')
    core = lax.rem(lax.axis_index('tp'), 2)
    same_core = [list(range(start, size, 2)) for start in range(2)]
    partner = [(index, index ^ 1) for index in range(size)]
    dim = patch_w.shape[1]
    heads_here, width = qkv_w.shape[2:]
    heads_half = heads_here * size // 2
    head_rows = heads_here * width
    scale = width ** -0.5
    cols_here = fc1_w.shape[1]
    cols_pad = round_up(cols_here, 32)
    ln_scale_f = ln_scale.astype(WIDE)
    ln_bias_f = ln_bias.astype(WIDE)
    tie = lax.optimization_barrier

    def images_of(x_val):
        x_val = x_val.reshape(size, -1, *x_val.shape[1:])
        return lax.all_to_all(x_val, 'tp', 0, 0, tiled=True)

    def gather(x_val, axis):
        return lax.all_gather(x_val, 'tp', axis=axis, tiled=True, axis_index_groups=same_core)

    def swap(x_val):
        return lax.ppermute(x_val, 'tp', partner)

    def scatter(x_val, axis):
        return lax.psum_scatter(x_val, 'tp', scatter_dimension=axis, tiled=True, axis_index_groups=same_core)

    def halves_of(table):
        table = table.reshape(size // 2, 2, *table.shape[1:])
        return [lax.dynamic_index_in_dim(table, index, 1, keepdims=False) for index in (core, 1 - core)]

    def product(spec, a_val, b_val):
        return jnp.einsum(spec, a_val, b_val, preferred_element_type=WIDE)

    def summed(spec, a_pair, b_pair):
        return product(spec, a_pair[0], b_pair[0]) + product(spec, a_pair[1], b_pair[1])

    def chip_product(spec, left, left_partner, right, right_partner):
        return product(spec, left_partner, right_partner) + tie(product(spec, left, right))

    pos_rows = pos_emb.shape[0]
    biases = jnp.concatenate([qkv_b.reshape(-1), fc1_b])
    biases = jnp.pad(biases, (0, dim - biases.shape[0]))[None]
    tables = pad_rows(jnp.concatenate([pos_emb, biases]), round_up(pos_rows + 1, 16))
    patches_img = images_of(patches)
    tables = lax.all_gather(tables, 'tp', axis=0)
    pos_all = tables[:, :pos_rows]
    qkv_b_all = [part.reshape(-1, 3, head_rows).transpose(1, 0, 2).reshape(3, 1, 1, 1, -1).astype(WIDE)
                 for part in halves_of(tables[:, pos_rows, :3 * head_rows])]
    fc1_b_all = [jnp.pad(part, ((0, 0), (0, cols_pad - cols_here))).reshape(-1).astype(WIDE)
                 for part in halves_of(tables[:, pos_rows, 3 * head_rows:3 * head_rows + cols_here])]
    attention_rows = jnp.concatenate([qkv_w.transpose(0, 2, 3, 1).reshape(3, head_rows, dim), out_w.reshape(1, head_rows, dim)])
    attention_own = gather(attention_rows, 1)
    fc1_own = gather(pad_rows(fc1_w.T, cols_pad), 0)
    d_out_img = images_of(d_out)
    fc2_own = gather(pad_rows(fc2_w, cols_pad), 0)

    emb = product('gbtp,pd->gbtd', patches_img, patch_w)
    emb_f = (emb + patch_b.astype(WIDE) + pos_all[:, None].astype(WIDE)).astype(HALF).astype(WIDE)
    h_one_f, ln_one_vjp = jax.vjp(layer_norm, emb_f, ln_scale_f[0], ln_bias_f[0])
    h_one = h_one_f.astype(HALF)
    attention_own, h_one = tie((attention_own, h_one))
    attention_all = [attention_own, swap(attention_own)]
    qkv_all = [part[:3] for part in attention_all]
    out_all = [part[3] for part in attention_all]
    qkv = [(product('gbtd,snd->sgbtn', h_one, weight) + bias).astype(HALF) for weight, bias in zip(qkv_all, qkv_b_all)]
    h_one_partner = swap(h_one)
    context = [attention_forward(part, heads_half, scale) for part in qkv]
    attn_out = summed('gbtn,nd->gbtd', context, out_all)
    x_one_f = (emb_f + (attn_out + out_b.astype(WIDE))).astype(HALF).astype(WIDE)
    h_two_f, ln_two_vjp = jax.vjp(layer_norm, x_one_f, ln_scale_f[1], ln_bias_f[1])
    h_two = h_two_f.astype(HALF)
    d_out_img, x_one_f = tie((d_out_img, x_one_f))
    d_out_partner = swap(d_out_img)
    fc1_own, h_two, d_out_img, d_out_partner = tie((fc1_own, h_two, d_out_img, d_out_partner))
    h_two_partner = swap(h_two)
    fc1_all = [fc1_own, swap(fc1_own)]
    hidden, gelu_vjps, rows = [], [], h_two
    for weight, bias in zip(fc1_all, fc1_b_all):
        hidden_f, gelu_vjp = jax.vjp(gelu_tanh, product('gbtd,fd->gbtf', rows, weight) + bias)
        hidden_h, rows = tie((hidden_f.astype(HALF), rows))
        hidden.append(hidden_h)
        gelu_vjps.append(gelu_vjp)


    d_fc2_b = jnp.sum(d_out.astype(WIDE), axis=(0, 1))
    grad_fc2 = chip_product('gbtf,gbtd->fd', hidden[0], swap(hidden[1]), d_out_img, d_out_partner)
    grad_fc2, d_out_img, fc2_own, hidden = tie((grad_fc2, d_out_img, fc2_own, hidden))
    fc2_all = [fc2_own, swap(fc2_own)]
    d_fc2_w = scatter(grad_fc2, 0)
    d_pre, d_fc1_b, rows = [], [], d_out_img
    for gelu_vjp, weight in zip(gelu_vjps, fc2_all):
        part = gelu_vjp(product('gbtd,fd->gbtf', rows, weight).astype(HALF).astype(WIDE))[0]
        d_fc1_b.append(jnp.sum(part, axis=(0, 1, 2)))
        part, rows = tie((part.astype(HALF), rows))
        d_pre.append(part)
    d_h_two = summed('gbtf,fd->gbtd', d_pre, fc1_all).astype(HALF)
    d_pre_partner = swap(d_pre[1])
    d_h_two, d_pre, d_pre_partner, hidden = tie((d_h_two, d_pre, d_pre_partner, hidden))
    x_two = (x_one_f + (summed('gbtf,fd->gbtd', hidden, fc2_all) + fc2_b.astype(WIDE))).astype(HALF)
    x_two, d_pre, d_pre_partner = tie((x_two, d_pre, d_pre_partner))
    x_two = lax.all_to_all(x_two, 'tp', 0, 0, tiled=True).reshape(d_out.shape)
    grad_fc1 = chip_product('gbtf,gbtd->fd', d_pre[0], d_pre_partner, h_two, h_two_partner)
    grad_fc1, d_h_two = tie((grad_fc1, d_h_two))
    d_fc1_w = scatter(grad_fc1, 0)
    d_x_ln, d_ln2_scale, d_ln2_bias = ln_two_vjp(d_h_two.astype(WIDE))
    d_x_one = (d_out_img.astype(WIDE) + d_x_ln).astype(HALF)
    d_out_b = jnp.sum(d_x_one, axis=(0, 1, 2), dtype=WIDE)
    d_context = [product('gbtd,nd->gbtn', d_x_one, weight).astype(HALF) for weight in out_all]
    d_x_partner, context_partner = swap(d_x_one), swap(context[1])
    d_context, d_fc2_w = tie((d_context, d_fc2_w))
    d_qkv = [attention_backward(*args, heads_half, scale) for args in zip(qkv[::-1], d_context[::-1])][::-1]
    d_x_partner, context_partner, d_qkv, x_two = tie((d_x_partner, context_partner, d_qkv, x_two))
    d_qkv_partner = swap(d_qkv[1])
    grad_out = chip_product('gbtn,gbtd->nd', context[0], context_partner, d_x_one, d_x_partner)
    grad_out, d_qkv, d_qkv_partner = tie((grad_out, d_qkv, d_qkv_partner))
    grad_qkv, d_qkv_partner = tie((product('sgbtn,gbtd->snd', d_qkv[0], h_one), d_qkv_partner))
    grad_qkv = grad_qkv + product('sgbtn,gbtd->snd', d_qkv_partner, h_one_partner)
    grad_qkv, grad_out, d_qkv = tie((grad_qkv, grad_out, d_qkv))
    grad_attention = scatter(jnp.concatenate([grad_qkv, grad_out[None]]), 1)
    d_h_one = summed('sgbtn,snd->gbtd', d_qkv, qkv_all).astype(HALF)
    d_qkv_b = [jnp.sum(part, axis=(1, 2, 3), dtype=WIDE) for part in d_qkv]
    d_emb_ln, d_ln1_scale, d_ln1_bias = ln_one_vjp(d_h_one.astype(WIDE))
    d_emb = (d_x_one.astype(WIDE) + d_emb_ln).astype(HALF)
    d_pos = jnp.sum(d_emb, axis=1, dtype=WIDE)
    d_patch_b = jnp.sum(d_emb, axis=(0, 1, 2), dtype=WIDE)
    d_patch_w = product('gbtp,gbtd->pd', patches_img, d_emb)

    d_fc1_w = d_fc1_w[:cols_here].astype(HALF).T
    d_patch_w, d_fc1_w = tie((d_patch_w, d_fc1_w))
    biases = [jnp.concatenate([fc1_part.reshape(size // 2, -1), qkv_part.reshape(3, size // 2, -1).transpose(1, 0, 2).reshape(size // 2, -1)], axis=1)
              for fc1_part, qkv_part in zip(d_fc1_b, d_qkv_b)]
    biases = jnp.where(core == 0, jnp.stack(biases, axis=1), jnp.stack(biases[::-1], axis=1)).reshape(size, -1)
    d_ln_scale = jnp.stack([d_ln1_scale, d_ln2_scale])
    d_ln_bias = jnp.stack([d_ln1_bias, d_ln2_bias])
    small = (d_patch_w, d_patch_b, d_ln_scale, d_ln_bias, d_out_b, d_fc2_b, d_pos, biases)
    small = [part.astype(HALF) for part in lax.psum(small, 'tp')]
    d_patch_w, d_patch_b, d_ln_scale, d_ln_bias, d_out_b, d_fc2_b, d_pos, biases = small
    d_pos, biases = [lax.dynamic_index_in_dim(part, lax.axis_index('tp'), 0, keepdims=False) for part in (d_pos, biases)]
    d_fc1_b = biases[:cols_here]
    d_qkv_b = biases[cols_pad:].reshape(3, heads_here, width)

    d_qkv_w = grad_attention[:3].astype(HALF).reshape(3, heads_here, width, dim).transpose(0, 3, 1, 2)
    d_out_w = grad_attention[3].astype(HALF).reshape(heads_here, width, dim)
    d_fc2_w = d_fc2_w[:cols_here].astype(HALF)
    return (x_two, d_patch_w, d_patch_b, d_pos, d_ln_scale, d_ln_bias, d_qkv_w, d_qkv_b, d_out_w, d_out_b, d_fc1_w, d_fc1_b, d_fc2_w, d_fc2_b)


def solution(mesh):
    in_specs = (P('dp', 'tp', None), P(), P(), P('tp', None), P(), P(), P(None, None, 'tp', None), P(None, 'tp', None), P('tp', None, None), P(), P(None, 'tp'), P('tp'), P('tp', None), P(), P('dp', 'tp', None))
    out_specs = (P('dp', 'tp', None), P('dp', None), P('dp'), P(('dp', 'tp'), None), P('dp', None), P('dp', None), P('dp', None, 'tp', None), P('dp', 'tp', None), P(('dp', 'tp'), None, None), P('dp'), P('dp', 'tp'), P(('dp', 'tp')), P(('dp', 'tp'), None), P('dp'))
    return jax.shard_map(group_step, mesh=mesh, in_specs=in_specs, out_specs=out_specs, check_vma=False)
```
